32 devices in a mesh: mode: 4 (over y, x), mesh: 8 (over z, core).
Axes of the slice: x: 2, y: 2, z: 4, core: 2. Of those that a mesh axis runs over, the one named last changes fastest.
Arguments:
- velocity: float32 [3, 2, 64, 20480], P(None, None, 'mode', 'mesh'), may hold values from -2.1 to 2.1
- magnetic: float32 [3, 2, 64, 20480], P(None, None, 'mode', 'mesh'), may hold values from -2.1 to 2.1
- leaf_inverse: bfloat16 [64, 160, 128, 128], P('mode', 'mesh'), may hold values from -1 to 2
- leaf_coupling: bfloat16 [64, 128, 20480], P('mode', None, 'mesh'), may hold values from -0.05908203 to 0.05908203
- separator_inverse: bfloat16 [64, 1024, 128], P('mode', 'mesh'), may hold values from -1 to 2
- separator_coupling: bfloat16 [64, 1024, 128], P('mode', 'mesh'), may hold values from -0.26367188 to 0.26367188
- separator_source: float32 [2, 64, 1024], P(None, 'mode', 'mesh'), may hold values from -6 to 6
- front_rows: int32 [8, 2, 128], P('mesh'), may hold values from 0 to 127, each once within a row
Outputs:
- nonlinear: float32 [3, 2, 64, 20480], P(None, None, 'mode', 'mesh')
- azimuthal_field: float32 [2, 64, 20480], P(None, 'mode', 'mesh')
- separator_solution: float32 [2, 64, 1024], P(None, 'mode', 'mesh')
The draws below stay inside these ranges and needn't reach their ends.
Inputs may be any that keep to these rules, and one draw needn't show every extreme that they name: front_rows[p, 0] and front_rows[p, 1] each hold every number below 128 once.
All inputs are finite; a program needn't handle non-finite values.
Results may differ from the reference program's by a relative error of at most 0.015.
Values may be sent and summed in bfloat16 or wider, within the bound.
No kernel may reach another device: no remote copies, remote signals or barrier semaphores. Data moves between devices by JAX's collectives and lax.ppermute only.
A program may use at most 128 MiB of HBM per device.

```python
import jax
import jax.numpy as jnp
from jax import lax

M = 64
NPHI = 192
NB = 128
NS = 128
ND = 2560
KB = 20
NODES = 20480
LEVELS = 3
N_MESH = 8


def draw_leaf_inverse(key, part):
    shape = (M, NODES // NB, NB, NB)
    identity = jnp.eye(NB, dtype=jnp.float32)
    values = identity + jax.random.truncated_normal(key, -4.0, 4.0, shape, jnp.float32) * (0.5 / NB ** 0.5)
    return values.astype(jnp.bfloat16)


def draw_separator_inverse(key, part):
    shape = (M, N_MESH, NS, NS)
    identity = jnp.eye(NS, dtype=jnp.float32)
    values = identity + jax.random.truncated_normal(key, -4.0, 4.0, shape, jnp.float32) * (0.5 / NS ** 0.5)
    return values.reshape(M, N_MESH * NS, NS).astype(jnp.bfloat16)


def steps_of(key, extent, shards, least, largest):
    def one(axis_at, blocks):
        heights = jax.random.uniform(jax.random.fold_in(jax.random.fold_in(key, 6), axis_at), (blocks,), jnp.float32, least / len(shards), largest / len(shards))
        return jnp.repeat(jnp.exp(heights), extent[axis_at] // blocks).reshape((-1,) + (1,) * (len(extent) - axis_at - 1))

    level = one(*shards[0])
    for cut in shards[1:]:
        level = level * one(*cut)
    return level


def scatter_about(key, dims, spread, reach, pieces=(), held_as=jnp.bfloat16):
    result = jax.random.normal(key, dims, jnp.float32) * spread
    if len(pieces) > 0:
        result = steps_of(key, dims, pieces, -0.22, 0.18) * result
    return jnp.clip(result, min=-reach, max=reach).astype(held_as)


def setup_inputs(seed: int = 0) -> dict:
    arg_keys = jax.random.split(jax.random.key(seed), 9)
    return {
        "velocity": scatter_about(arg_keys[0], (3, 2, M, NODES), 0.35, 2.1, ((2, 4), (3, 8)), jnp.float32),
        "magnetic": scatter_about(arg_keys[1], (3, 2, M, NODES), 0.35, 2.1, ((2, 4), (3, 8)), jnp.float32),
        "leaf_inverse": draw_leaf_inverse(jax.random.fold_in(arg_keys[8], 71), 0),
        "leaf_coupling": scatter_about(arg_keys[3], (M, NS, NODES), (0.5 * ND ** -0.5), 0.05908203, ((0, 4), (2, 8))),
        "separator_inverse": draw_separator_inverse(jax.random.fold_in(arg_keys[8], 71), 0),
        "separator_coupling": scatter_about(arg_keys[5], (M, N_MESH * NS, NS), (0.5 * NS ** -0.5), 0.26367188, ((0, 4), (1, 8))),
        "separator_source": scatter_about(arg_keys[6], (2, M, N_MESH * NS), 1.0, 6.0, ((1, 4), (2, 8)), jnp.float32),
        "front_rows": jax.vmap(lambda own: jax.random.permutation(own, NS))(jax.random.split(arg_keys[7], N_MESH * 2)).reshape((N_MESH, 2, NS)).astype(jnp.int32),
    }


highest = lax.Precision.HIGHEST
dt_step = 0.5


def tables():
    angles = jnp.arange(NPHI, dtype=jnp.int32)[:, None]
    orders = jnp.arange(M, dtype=jnp.int32)[None, :]
    phase = ((angles * orders) % NPHI).astype(jnp.float32) * (2.0 * jnp.pi / NPHI)
    forward = jnp.stack([jnp.cos(phase), jnp.sin(phase)], axis=1)
    weights = jnp.where(orders == 0, 1.0, 2.0).astype(jnp.float32) / NPHI
    backward = jnp.stack([(jnp.cos(phase) * weights).T, (jnp.sin(phase) * weights).T], axis=0)
    return forward, backward


def cross_terms(first, second):
    return jnp.stack([first[1] * second[2] - first[2] * second[1],
                      first[2] * second[0] - first[0] * second[2],
                      first[0] * second[1] - first[1] * second[0]])


def transform(forward, backward, velocity, magnetic):
    phys_velocity = jnp.einsum("kam,camn->ckn", forward, velocity, precision=highest)
    phys_magnetic = jnp.einsum("kam,camn->ckn", forward, magnetic, precision=highest)
    crossed = cross_terms(phys_velocity, phys_magnetic)
    return jnp.einsum("amk,ckn->camn", backward, crossed, precision=highest)


def rounded(values):
    return lax.optimization_barrier(values.astype(jnp.bfloat16)).astype(jnp.float32)


def forward_apply(matrix, vector):
    return jnp.einsum("mij,cmj->cmi", matrix.astype(jnp.float32), vector.astype(jnp.float32))


def transpose_apply(matrix, vector):
    return jnp.einsum("mij,cmi->cmj", matrix.astype(jnp.float32), vector.astype(jnp.float32))


def block_apply(factor, vector, form):
    shaped = vector.astype(jnp.float32).reshape(2, M, -1, NB)
    return jnp.einsum(form, factor.astype(jnp.float32), shaped).reshape(2, M, -1)


def level_of(owner):
    if owner == 0:
        return LEVELS + 1
    return (owner & -owner).bit_length()


def reference(velocity, magnetic, leaf_inverse, leaf_coupling, separator_inverse, separator_coupling, separator_source, front_rows):
    forward, backward = tables()
    pieces_out = []
    for block in range(N_MESH):
        node_span = slice(block * ND, (block + 1) * ND)
        pieces_out.append(transform(forward, backward, velocity[..., node_span], magnetic[..., node_span]))
    nonlinear = jnp.concatenate(pieces_out, axis=3)
    source = (magnetic[1] + dt_step * nonlinear[1]).astype(jnp.bfloat16)

    def leaf_parts(block):
        node_span = slice(block * ND, (block + 1) * ND)
        factor = leaf_inverse[:, block * KB:(block + 1) * KB]
        leaf_map = jnp.take(leaf_coupling[:, :, node_span], front_rows[block, 0], axis=1)
        return node_span, factor, leaf_map

    leaf_solved = []
    leaf_updates = []
    for block in range(N_MESH):
        node_span, factor, leaf_map = leaf_parts(block)
        solved = block_apply(factor, source[:, :, node_span], "mkij,cmkj->cmki").astype(jnp.bfloat16)
        leaf_solved.append(solved)
        leaf_updates.append(forward_apply(leaf_map, solved))

    def separator_parts(owner):
        row_span = slice(owner * NS, (owner + 1) * NS)
        inverse = separator_inverse[:, row_span]
        upward = jnp.take(separator_coupling[:, row_span], front_rows[owner, 1], axis=1)
        return inverse, upward, separator_source[:, :, row_span]

    reduced = {}
    outgoing = {}
    for height in range(1, LEVELS + 2):
        for owner in range(N_MESH):
            if level_of(owner) != height:
                continue
            if height == 1:
                arrived = leaf_updates[owner - 1] + leaf_updates[owner]
            elif height <= LEVELS:
                gap = 2 ** (height - 2)
                arrived = outgoing[owner - gap] + outgoing[owner + gap]
            else:
                arrived = outgoing[N_MESH // 2]
            inverse, upward, source_part = separator_parts(owner)
            reduced[owner] = forward_apply(inverse, rounded(source_part - arrived)).astype(jnp.bfloat16)
            outgoing[owner] = forward_apply(upward, reduced[owner])

    solution = {}
    inverse, upward, source_part = separator_parts(0)
    solution[0] = transpose_apply(inverse, reduced[0])
    for height in range(LEVELS, 0, -1):
        for owner in range(N_MESH):
            if level_of(owner) != height:
                continue
            if height == LEVELS:
                parent = 0
            else:
                parent = ((owner >> (height + 1)) << (height + 1)) + 2 ** height
            inverse, upward, source_part = separator_parts(owner)
            residue = reduced[owner].astype(jnp.float32) - transpose_apply(upward, rounded(solution[parent]))
            solution[owner] = transpose_apply(inverse, rounded(residue))
    separator_solution = jnp.concatenate([solution[owner] for owner in range(N_MESH)], axis=2)

    azimuthal = []
    for block in range(N_MESH):
        node_span, factor, leaf_map = leaf_parts(block)
        parent = 2 * (block // 2) + 1
        residue = leaf_solved[block].astype(jnp.float32) - transpose_apply(leaf_map, rounded(solution[parent]))
        azimuthal.append(block_apply(factor, rounded(residue), "mkji,cmkj->cmki"))
    azimuthal_field = jnp.concatenate(azimuthal, axis=2)
    return nonlinear, azimuthal_field, separator_solution
```

```python
import functools

import jax
import jax.numpy as jnp
from jax import lax
from jax.experimental import pallas as pl
from jax.experimental.pallas import tpu as pltpu
from jax.sharding import PartitionSpec as P

NPHI = 192
DT_STEP = 0.5
VMEM = pltpu.VMEM
SMEM = pltpu.SMEM
BF16 = jnp.bfloat16
F32 = jnp.float32
NT = (((1,), (1,)), ((), ()))
NN = (((1,), (0,)), ((), ()))


def dot(a, b, dims=NN, precision=None):
    return lax.dot_general(a, b, dims, precision=precision, preferred_element_type=F32)


def tables(me, groups, modes_dev):
    steps = jnp.bitwise_xor(me, jnp.arange(groups, dtype=jnp.int32))
    orders = (steps[:, None] * modes_dev + jnp.arange(modes_dev, dtype=jnp.int32)[None, :])[:, None, :]
    angles = jnp.arange(NPHI, dtype=jnp.int32)[:, None, None, None]
    phase = (angles * orders[None] % NPHI).astype(F32) * (2.0 * jnp.pi / NPHI)
    forward = jnp.concatenate([jnp.cos(phase), jnp.sin(phase)], axis=2)
    weights = jnp.where(orders == 0, 1.0, 2.0).astype(F32)[None] / NPHI
    rows = groups * 2 * modes_dev
    return (
        forward.reshape(NPHI, rows).astype(BF16),
        (forward * weights).reshape(NPHI, rows).T.astype(BF16),
    )


def pack_kernel(groups, me_ref, v_ref, b_ref, *outs):
    rows, width = v_ref.shape[0], outs[0].shape[1]
    for k in range(groups):
        span = pl.ds(pl.multiple_of(jnp.bitwise_xor(me_ref[0], k) * width, 128), width)
        outs[k][:rows, :] = v_ref[:, span].astype(BF16)
        outs[k][rows:, :] = b_ref[:, span].astype(BF16)


def pack(me, velocity, magnetic, groups):
    rows, nodes = velocity.shape
    width = nodes // groups
    return pl.pallas_call(
        functools.partial(pack_kernel, groups),
        out_shape=[jax.ShapeDtypeStruct((2 * rows, width), BF16)] * groups,
        in_specs=[pl.BlockSpec(memory_space=SMEM)] + [pl.BlockSpec(memory_space=VMEM)] * 2,
        out_specs=[pl.BlockSpec(memory_space=VMEM)] * groups,
        compiler_params=pltpu.CompilerParams(vmem_limit_bytes=16 * 2**20),
        name="pack",
    )(me, velocity, magnetic)


def transform_kernel(groups, fwd_ref, bwd_ref, *refs):
    ins, azi, rest = refs[:groups], refs[groups : 2 * groups], refs[2 * groups :]
    rows = ins[0].shape[0] // 6
    fwd, bwd = fwd_ref[...], bwd_ref[...]
    phys = []
    for field in range(6):
        coef = jnp.concatenate([r[field * rows : (field + 1) * rows, :] for r in ins], axis=0)
        phys.append(dot(fwd, coef))
    v, b = phys[:3], phys[3:]
    for c in range(3):
        p, q = (c + 1) % 3, (c + 2) % 3
        crossed = (v[p] * b[q] - v[q] * b[p]).astype(BF16)
        terms = dot(bwd, crossed).astype(BF16)
        for k in range(groups):
            block = terms[k * rows : (k + 1) * rows, :]
            if c == 1:
                azi[k][...] = block
            else:
                at = 0 if c == 0 else rows
                rest[k][at : at + rows, :] = block


def transform(fwd, bwd, pieces):
    groups = len(pieces)
    rows, width = pieces[0].shape
    rows = rows // 6
    out = pl.pallas_call(
        functools.partial(transform_kernel, groups),
        out_shape=[jax.ShapeDtypeStruct((rows, width), BF16)] * groups
        + [jax.ShapeDtypeStruct((2 * rows, width), BF16)] * groups,
        in_specs=[pl.BlockSpec(memory_space=VMEM)] * (2 + groups),
        out_specs=[pl.BlockSpec(memory_space=VMEM)] * (2 * groups),
        compiler_params=pltpu.CompilerParams(vmem_limit_bytes=24 * 2**20),
        name="transform",
    )(fwd, bwd, *pieces)
    return out[:groups], out[groups:]


def one_hot(rows_ref):
    n = rows_ref.shape[1]
    return lax.broadcasted_iota(jnp.int32, (n, n), 0) == rows_ref[0:1, :]


def fetch(modes, pairs, sems):
    def copy(which, m):
        src, dst = pairs[which]
        return pltpu.make_async_copy(src.at[m], dst.at[m], sems.at[which, m])

    def start(m, carry):
        for which in range(len(pairs)):
            copy(which, m).start()
        return carry

    lax.fori_loop(0, modes, start, 0)
    return copy


def leaf_up_kernel(groups, me_ref, rows_ref, mag_ref, *refs):
    pieces = refs[:groups]
    inv_hbm, cpl_hbm, solved_ref, update_ref, inv_v, cpl_v, src_v, upd_v, sems = refs[groups:]
    _, modes, nodes = mag_ref.shape
    width = nodes // groups
    blocks, size = inv_v.shape[1], inv_v.shape[2]
    copy = fetch(modes, ((inv_hbm, inv_v), (cpl_hbm, cpl_v)), sems)
    for k in range(groups):
        span = pl.ds(pl.multiple_of(jnp.bitwise_xor(me_ref[0], k) * width, 128), width)
        for a in range(2):
            term = pieces[k][a * modes : (a + 1) * modes, :].astype(F32)
            src_v[a, :, span] = (mag_ref[a, :, span] + DT_STEP * term).astype(BF16).astype(F32)

    def one_mode(m, carry):
        copy(0, m).wait()
        source = src_v[:, pl.ds(m, 1), :].reshape(2, nodes).astype(BF16)
        solved = jnp.concatenate(
            [
                dot(source[:, b * size : (b + 1) * size], inv_v[m, b], NT)
                for b in range(blocks)
            ],
            axis=1,
        ).astype(BF16)
        solved_ref[:, pl.ds(m, 1), :] = solved.astype(F32).reshape(2, 1, nodes)
        copy(1, m).wait()
        upd_v[:, pl.ds(m, 1), :] = dot(solved, cpl_v[m], NT).reshape(2, 1, size)
        return carry

    lax.fori_loop(0, modes, one_mode, 0)
    select = one_hot(rows_ref).astype(F32)
    for a in range(2):
        update_ref[a] = dot(upd_v[a], select, precision=lax.Precision.HIGHEST)


def leaf_up(me, rows, mag, pieces, inverse, coupling):
    _, modes, nodes = mag.shape
    groups = len(pieces)
    front = coupling.shape[1]
    any_spec, vmem_spec = pl.BlockSpec(memory_space=pl.ANY), pl.BlockSpec(memory_space=VMEM)
    return pl.pallas_call(
        functools.partial(leaf_up_kernel, groups),
        out_shape=[
            jax.ShapeDtypeStruct((2, modes, nodes), F32),
            jax.ShapeDtypeStruct((2, modes, front), F32),
        ],
        in_specs=[pl.BlockSpec(memory_space=SMEM)] + [vmem_spec] * (2 + groups) + [any_spec] * 2,
        out_specs=[vmem_spec] * 2,
        scratch_shapes=[
            VMEM(inverse.shape, BF16),
            VMEM(coupling.shape, BF16),
            VMEM((2, modes, nodes), F32),
            VMEM((2, modes, front), F32),
            pltpu.SemaphoreType.DMA((2, modes)),
        ],
        compiler_params=pltpu.CompilerParams(vmem_limit_bytes=48 * 2**20),
        name="leaf_up",
    )(me, rows, mag, *pieces, inverse, coupling)


def leaf_down_kernel(rows_ref, above_ref, solved_ref, inv_hbm, cpl_hbm, out_ref, inv_v, cpl_v, x_v, sems):
    _, modes, nodes = solved_ref.shape
    blocks, size = inv_v.shape[1], inv_v.shape[2]
    copy = fetch(modes, ((inv_hbm, inv_v), (cpl_hbm, cpl_v)), sems)
    select = one_hot(rows_ref).astype(F32).astype(BF16)
    for a in range(2):
        x_v[a] = dot(above_ref[a].astype(BF16), select, NT)

    def one_mode(m, carry):
        copy(1, m).wait()
        x = x_v[:, pl.ds(m, 1), :].reshape(2, size).astype(BF16)
        residue = (solved_ref[:, pl.ds(m, 1), :].reshape(2, nodes) - dot(x, cpl_v[m])).astype(BF16)
        copy(0, m).wait()
        field = jnp.concatenate(
            [dot(residue[:, b * size : (b + 1) * size], inv_v[m, b]) for b in range(blocks)],
            axis=1,
        )
        out_ref[:, pl.ds(m, 1), :] = field.reshape(2, 1, nodes)
        return carry

    lax.fori_loop(0, modes, one_mode, 0)


def leaf_down(rows, above, solved, inverse, coupling):
    any_spec, vmem_spec = pl.BlockSpec(memory_space=pl.ANY), pl.BlockSpec(memory_space=VMEM)
    modes = solved.shape[1]
    return pl.pallas_call(
        leaf_down_kernel,
        out_shape=jax.ShapeDtypeStruct(solved.shape, F32),
        in_specs=[vmem_spec] * 3 + [any_spec] * 2,
        out_specs=vmem_spec,
        scratch_shapes=[
            VMEM(inverse.shape, BF16),
            VMEM(coupling.shape, BF16),
            VMEM(above.shape, F32),
            pltpu.SemaphoreType.DMA((2, modes)),
        ],
        compiler_params=pltpu.CompilerParams(vmem_limit_bytes=48 * 2**20),
        name="leaf_down",
    )(rows, above, solved, inverse, coupling)


def spread_kernel(groups, me_ref, *refs):
    azi, rest, out_ref = refs[:groups], refs[groups : 2 * groups], refs[2 * groups]
    rows, width = azi[0].shape
    for k in range(groups):
        span = pl.ds(pl.multiple_of(jnp.bitwise_xor(me_ref[0], k) * width, 128), width)
        out_ref[:rows, span] = rest[k][:rows, :].astype(F32)
        out_ref[rows : 2 * rows, span] = azi[k][...].astype(F32)
        out_ref[2 * rows :, span] = rest[k][rows:, :].astype(F32)


def spread(me, azi, rest):
    groups = len(azi)
    rows, width = azi[0].shape
    return pl.pallas_call(
        functools.partial(spread_kernel, groups),
        out_shape=jax.ShapeDtypeStruct((3 * rows, groups * width), F32),
        in_specs=[pl.BlockSpec(memory_space=SMEM)] + [pl.BlockSpec(memory_space=VMEM)] * (2 * groups),
        out_specs=pl.BlockSpec(memory_space=VMEM),
        compiler_params=pltpu.CompilerParams(vmem_limit_bytes=16 * 2**20),
        name="spread",
    )(me, *azi, *rest)


def level_of(q, levels):
    return levels + 1 if q == 0 else (q & -q).bit_length()


def shards(
    velocity,
    magnetic,
    leaf_inverse,
    leaf_coupling,
    separator_inverse,
    separator_coupling,
    separator_source,
    front_rows,
):
    groups = lax.axis_size("mode")
    partitions = lax.axis_size("mesh")
    levels = partitions.bit_length() - 1
    modes, nodes = velocity.shape[2], velocity.shape[3]
    sep_rows = separator_source.shape[2]
    here = lax.axis_index("mode")
    me = here.reshape(1).astype(jnp.int32)
    position = lax.axis_index("mesh")
    exchange = [[(g, g ^ k) for g in range(groups)] for k in range(groups)]

    def swap(pieces):
        return [pieces[0]] + [
            lax.ppermute(pieces[k], "mode", exchange[k]) for k in range(1, groups)
        ]

    fwd, bwd = tables(here, groups, modes)
    packed = pack(me, velocity.reshape(6 * modes, nodes), magnetic.reshape(6 * modes, nodes), groups)
    azi, rest = transform(fwd, bwd, swap(packed))
    azi = swap(azi)
    rest = swap(rest)
    row_order = front_rows[0]
    solved, update = leaf_up(me, row_order[0:1], magnetic[1], azi, leaf_inverse, leaf_coupling)
    nonlinear = spread(me, azi, rest).reshape(3, 2, modes, nodes)

    select = (jnp.arange(sep_rows, dtype=jnp.int32)[:, None] == row_order[1][None, :]).astype(F32)
    level_here = sum((position % 2**t == 0).astype(jnp.int32) for t in range(1, levels + 1)) + 1
    of_level = [[q for q in range(partitions) if level_of(q, levels) == h] for h in range(levels + 2)]

    def settle(arrived, height, reduced, outgoing):
        fresh = jnp.einsum(
            "mij,cmj->cmi",
            separator_inverse,
            (separator_source - arrived).astype(BF16),
            preferred_element_type=F32,
        ).astype(BF16)
        active = level_here == height
        reduced = jnp.where(active, fresh, reduced)
        if height <= levels:
            sending = jnp.einsum("mij,cmj->cmi", separator_coupling, fresh, preferred_element_type=F32)
            sending = jnp.einsum(
                "cmj,ji->cmi", sending, select, precision=lax.Precision.HIGHEST,
                preferred_element_type=F32,
            )
            outgoing = jnp.where(active, sending, outgoing)
        return reduced, outgoing

    reduced = jnp.zeros(separator_source.shape, BF16)
    outgoing = jnp.zeros(separator_source.shape, F32)
    arrived = update + lax.ppermute(update, "mesh", [(q - 1, q) for q in of_level[1]])
    reduced, outgoing = settle(arrived, 1, reduced, outgoing)
    for height in range(2, levels + 1):
        gap = 2 ** (height - 2)
        arrived = lax.ppermute(outgoing, "mesh", [(q - gap, q) for q in of_level[height]])
        arrived += lax.ppermute(outgoing, "mesh", [(q + gap, q) for q in of_level[height]])
        reduced, outgoing = settle(arrived, height, reduced, outgoing)
    arrived = lax.ppermute(outgoing, "mesh", [(partitions // 2, 0)])
    reduced, outgoing = settle(arrived, levels + 1, reduced, outgoing)

    top = jnp.einsum("mij,cmi->cmj", separator_inverse, reduced, preferred_element_type=F32)
    solution = jnp.where(level_here == levels + 1, top, jnp.zeros(separator_source.shape, F32))
    for height in range(levels, 0, -1):
        sending = solution.astype(BF16)
        if height == levels:
            above = lax.ppermute(sending, "mesh", [(0, partitions // 2)])
        else:
            gap = 2 ** (height - 1)
            parents = of_level[height + 1]
            above = lax.ppermute(sending, "mesh", [(q, q - gap) for q in parents])
            above += lax.ppermute(sending, "mesh", [(q, q + gap) for q in parents])
        above = jnp.einsum(
            "cmi,ji->cmj", above, select.astype(BF16), preferred_element_type=F32
        ).astype(BF16)
        residue = reduced.astype(F32) - jnp.einsum(
            "mij,cmi->cmj", separator_coupling, above, preferred_element_type=F32
        )
        fresh = jnp.einsum(
            "mij,cmi->cmj", separator_inverse, residue.astype(BF16), preferred_element_type=F32
        )
        solution = jnp.where(level_here == height, fresh, solution)
    sending = solution.astype(BF16)
    beside = lax.ppermute(sending, "mesh", [(q, q - 1) for q in of_level[1]])
    above = jnp.where(level_here == 1, sending, beside)
    azimuthal = leaf_down(row_order[0:1], above.astype(F32), solved, leaf_inverse, leaf_coupling)
    return (nonlinear, azimuthal, solution)


def solution(mesh):
    in_specs = (
        P(None, None, "mode", "mesh"),
        P(None, None, "mode", "mesh"),
        P("mode", "mesh", None, None),
        P("mode", None, "mesh"),
        P("mode", "mesh", None),
        P("mode", "mesh", None),
        P(None, "mode", "mesh"),
        P("mesh", None, None),
    )
    out_specs = (P(None, None, "mode", "mesh"), P(None, "mode", "mesh"), P(None, "mode", "mesh"))
    return jax.shard_map(shards, mesh=mesh, in_specs=in_specs, out_specs=out_specs, check_vma=False)
```

```python
import functools

import jax
import jax.numpy as jnp
from jax import lax
from jax.experimental import pallas as pl
from jax.experimental.pallas import tpu as pltpu
from jax.sharding import PartitionSpec as P

NPHI = 192
DT_STEP = 0.5
VMEM = pltpu.VMEM
SMEM = pltpu.SMEM
BF16 = jnp.bfloat16
F32 = jnp.float32
NT = (((1,), (1,)), ((), ()))
NN = (((1,), (0,)), ((), ()))
SMALL = 8 * 2**20
LARGE = 8 * 2**20
COMPOSE = 8 * 2**20


def dot(a, b, dims=NN, precision=None):
    return lax.dot_general(a, b, dims, precision=precision, preferred_element_type=F32)


def tables_kernel(modes, me_ref, fwd_ref, bwd_ref):
    def phase(shape, angle_axis):
        angle = lax.broadcasted_iota(jnp.int32, shape, angle_axis)
        at = lax.broadcasted_iota(jnp.int32, shape, 1 - angle_axis)
        step, kind, mode = at // (2 * modes), (at // modes) % 2, at % modes
        order = jnp.bitwise_xor(step, me_ref[0]) * modes + mode
        turn = (angle * order).astype(F32)
        turn = turn - NPHI * jnp.floor((turn + 0.5) * (1.0 / NPHI))
        return turn * (2.0 * jnp.pi / NPHI), kind, order

    at, kind, _ = phase(fwd_ref.shape, 0)
    fwd_ref[...] = jnp.where(kind == 0, jnp.cos(at), jnp.sin(at)).astype(BF16)
    at, kind, order = phase(bwd_ref.shape, 1)
    weight = jnp.where(order == 0, 1.0, 2.0) / NPHI
    bwd_ref[...] = (jnp.where(kind == 0, jnp.cos(at), jnp.sin(at)) * weight).astype(BF16)


def tables(me, groups, modes):
    rows = groups * 2 * modes
    return pl.pallas_call(
        functools.partial(tables_kernel, modes),
        out_shape=[jax.ShapeDtypeStruct((NPHI, rows), BF16), jax.ShapeDtypeStruct((rows, NPHI), BF16)],
        in_specs=[pl.BlockSpec(memory_space=SMEM)],
        out_specs=[pl.BlockSpec(memory_space=VMEM)] * 2,
        compiler_params=pltpu.CompilerParams(vmem_limit_bytes=SMALL),
        name="tables",
    )(me)


def pack_kernel(groups, me_ref, v_ref, b_ref, *outs):
    rows, width = v_ref.shape[0], outs[0].shape[1]
    for k in range(groups):
        span = pl.ds(pl.multiple_of(jnp.bitwise_xor(me_ref[0], k) * width, 128), width)
        outs[k][:rows, :] = v_ref[:, span].astype(BF16)
        outs[k][rows:, :] = b_ref[:, span].astype(BF16)


def pack(me, velocity, magnetic, groups):
    rows, nodes = velocity.shape
    width = nodes // groups
    return pl.pallas_call(
        functools.partial(pack_kernel, groups),
        out_shape=[jax.ShapeDtypeStruct((2 * rows, width), BF16)] * groups,
        in_specs=[pl.BlockSpec(memory_space=SMEM)] + [pl.BlockSpec(memory_space=VMEM)] * 2,
        out_specs=[pl.BlockSpec(memory_space=VMEM)] * groups,
        compiler_params=pltpu.CompilerParams(vmem_limit_bytes=16 * 2**20),
        name="pack",
    )(me, velocity, magnetic)


def transform_kernel(groups, fwd_ref, bwd_ref, *refs):
    ins, azi, rest = refs[:groups], refs[groups : 2 * groups], refs[2 * groups :]
    rows = ins[0].shape[0] // 6
    fwd, bwd = fwd_ref[...], bwd_ref[...]
    phys = []
    for field in range(6):
        coef = jnp.concatenate([r[field * rows : (field + 1) * rows, :] for r in ins], axis=0)
        phys.append(dot(fwd, coef))
    v, b = phys[:3], phys[3:]
    for c in range(3):
        p, q = (c + 1) % 3, (c + 2) % 3
        crossed = (v[p] * b[q] - v[q] * b[p]).astype(BF16)
        terms = dot(bwd, crossed).astype(BF16)
        for k in range(groups):
            block = terms[k * rows : (k + 1) * rows, :]
            if c == 1:
                azi[k][...] = block
            else:
                at = 0 if c == 0 else rows
                rest[k][at : at + rows, :] = block


def transform(fwd, bwd, pieces):
    groups = len(pieces)
    rows, width = pieces[0].shape
    rows = rows // 6
    out = pl.pallas_call(
        functools.partial(transform_kernel, groups),
        out_shape=[jax.ShapeDtypeStruct((rows, width), BF16)] * groups
        + [jax.ShapeDtypeStruct((2 * rows, width), BF16)] * groups,
        in_specs=[pl.BlockSpec(memory_space=VMEM)] * (2 + groups),
        out_specs=[pl.BlockSpec(memory_space=VMEM)] * (2 * groups),
        compiler_params=pltpu.CompilerParams(vmem_limit_bytes=24 * 2**20),
        name="transform",
    )(fwd, bwd, *pieces)
    return out[:groups], out[groups:]


def one_hot(rows_ref):
    n = rows_ref.shape[1]
    return lax.broadcasted_iota(jnp.int32, (n, n), 0) == rows_ref[0:1, :]


def compose_kernel(inv_hbm, cpl_hbm, square_ref, joint_ref, inv_v, cpl_v, sems):
    modes, front, nodes = joint_ref.shape
    blocks, size = inv_v.shape[1], inv_v.shape[2]
    depth = inv_v.shape[0]
    zero = jnp.zeros((size, size), BF16)

    def copies(m):
        slot = m % depth
        return (
            pltpu.make_async_copy(inv_hbm.at[m], inv_v.at[slot], sems.at[0, slot]),
            pltpu.make_async_copy(cpl_hbm.at[m], cpl_v.at[slot], sems.at[1, slot]),
        )

    for m in range(depth):
        for copy in copies(m):
            copy.start()

    def one_mode(m, carry):
        slot = m % depth
        for copy in copies(m):
            copy.wait()
        for b in range(0, blocks, 2):
            first, second = inv_v[slot, b], inv_v[slot, b + 1]
            weights = jnp.concatenate(
                [jnp.concatenate([first, zero], axis=1), jnp.concatenate([zero, second], axis=1)],
                axis=0,
            )
            span = slice(b * size, (b + 2) * size)
            rows = jnp.concatenate(
                [cpl_v[slot, :, span], jnp.concatenate([first.T, second.T], axis=1)], axis=0
            )
            out = dot(rows, weights).astype(BF16)
            joint_ref[m, :, span] = out[:front]
            square_ref[m, b] = out[front:, :size]
            square_ref[m, b + 1] = out[front:, size:]

        @pl.when(m + depth < modes)
        def _():
            for copy in copies(m + depth):
                copy.start()

        return carry

    lax.fori_loop(0, modes, one_mode, 0)


def compose(inverse, coupling, depth=4):
    modes, blocks, size, _ = inverse.shape
    front, nodes = coupling.shape[1:]
    return pl.pallas_call(
        compose_kernel,
        out_shape=[
            jax.ShapeDtypeStruct(inverse.shape, BF16),
            jax.ShapeDtypeStruct(coupling.shape, BF16),
        ],
        in_specs=[pl.BlockSpec(memory_space=pl.ANY)] * 2,
        out_specs=[pl.BlockSpec(memory_space=VMEM)] * 2,
        scratch_shapes=[
            VMEM((depth, blocks, size, size), BF16),
            VMEM((depth, front, nodes), BF16),
            pltpu.SemaphoreType.DMA((2, depth)),
        ],
        compiler_params=pltpu.CompilerParams(vmem_limit_bytes=COMPOSE),
        cost_estimate=pl.CostEstimate(
            flops=4 * modes * nodes * size * (front + size),
            bytes_accessed=4 * (inverse.size + coupling.size),
            transcendentals=0,
        ),
        name="compose",
    )(inverse, coupling)


def leaf_up_kernel(groups, me_ref, rows_ref, mag_ref, joint_ref, *refs):
    pieces = refs[:groups]
    source_ref, update_ref, turned_v = refs[groups:]
    modes, front, nodes = joint_ref.shape
    width = nodes // groups
    for k in range(groups):
        span = pl.ds(pl.multiple_of(jnp.bitwise_xor(me_ref[0], k) * width, 128), width)
        for a in range(2):
            term = pieces[k][a * modes : (a + 1) * modes, :].astype(F32)
            source_ref[a, :, span] = mag_ref[0, a, :, span] + DT_STEP * term
    turned_v[...] = source_ref[...].reshape(2 * modes, nodes).T.astype(BF16)
    turned = turned_v[...]
    lane = lax.broadcasted_iota(jnp.int32, (front, 2 * modes), 1) % modes

    def one_mode(m, total):
        return total + jnp.where(lane == m, dot(joint_ref[m], turned), 0.0)

    total = lax.fori_loop(0, modes, one_mode, jnp.zeros((front, 2 * modes), F32), unroll=2)
    select = one_hot(rows_ref).astype(F32)
    update_ref[...] = dot(total.T, select, precision=lax.Precision.HIGHEST).reshape(update_ref.shape)


def leaf_up(me, rows, magnetic, pieces, joint):
    modes, front, nodes = joint.shape
    groups = len(pieces)
    whole = pl.BlockSpec(memory_space=VMEM)
    return pl.pallas_call(
        functools.partial(leaf_up_kernel, groups),
        grid=(1,),
        out_shape=[
            jax.ShapeDtypeStruct((2, modes, nodes), F32),
            jax.ShapeDtypeStruct((2, modes, front), F32),
        ],
        in_specs=[
            pl.BlockSpec(memory_space=SMEM),
            whole,
            pl.BlockSpec((1, 2, modes, nodes), lambda i: (1, 0, 0, 0)),
        ]
        + [whole] * (1 + groups),
        out_specs=[whole] * 2,
        scratch_shapes=[VMEM((nodes, 2 * modes), BF16)],
        compiler_params=pltpu.CompilerParams(vmem_limit_bytes=LARGE),
        cost_estimate=pl.CostEstimate(
            flops=128 * modes * nodes * front, bytes_accessed=2 * joint.size, transcendentals=0
        ),
        name="leaf_up",
    )(me, rows, magnetic, joint, *pieces)


def leaf_local_kernel(source_ref, square_ref, out_ref):
    modes, blocks, size, _ = square_ref.shape
    nodes = blocks * size
    zero = jnp.zeros((2, size), BF16)

    def one_mode(m, carry):
        source = source_ref[:, pl.ds(m, 1), :].reshape(2, nodes).astype(BF16)
        parts = []
        for b in range(0, blocks, 2):
            one = source[:, b * size : (b + 1) * size]
            two = source[:, (b + 1) * size : (b + 2) * size]
            left = jnp.concatenate(
                [jnp.concatenate([one, zero], axis=1), jnp.concatenate([zero, two], axis=1)], axis=0
            )
            pair = dot(left, square_ref[m, b : b + 2].reshape(2 * size, size))
            parts += [pair[:2], pair[2:]]
        out_ref[:, pl.ds(m, 1), :] = jnp.concatenate(parts, axis=1).reshape(2, 1, nodes)
        return carry

    lax.fori_loop(0, modes, one_mode, 0, unroll=2)


def leaf_local(source, square):
    whole = pl.BlockSpec(memory_space=VMEM)
    return pl.pallas_call(
        leaf_local_kernel,
        out_shape=jax.ShapeDtypeStruct(source.shape, F32),
        in_specs=[whole] * 2,
        out_specs=whole,
        compiler_params=pltpu.CompilerParams(vmem_limit_bytes=LARGE),
        cost_estimate=pl.CostEstimate(
            flops=128 * square.size, bytes_accessed=2 * square.size, transcendentals=0
        ),
        name="leaf_local",
    )(source, square)


def leaf_down_kernel(own_ref, rows_ref, here_ref, beside_ref, local_ref, joint_ref, out_ref, x_v):
    modes, front, nodes = joint_ref.shape
    select = one_hot(rows_ref).astype(F32).astype(BF16)
    above = jnp.where(own_ref[0] == 1, here_ref[...].astype(F32), beside_ref[...].astype(F32))
    x_v[...] = dot(above.reshape(2 * modes, front).astype(BF16), select, NT).reshape(2, modes, front)
    zero = jnp.zeros((2, front), F32)

    def two_modes(i, carry):
        one = x_v[:, pl.ds(2 * i, 1), :].reshape(2, front)
        two = x_v[:, pl.ds(2 * i + 1, 1), :].reshape(2, front)
        left = jnp.concatenate(
            [jnp.concatenate([one, zero], axis=1), jnp.concatenate([zero, two], axis=1)], axis=0
        ).astype(BF16)
        out = dot(left, joint_ref[pl.ds(2 * i, 2)].reshape(2 * front, nodes))
        for half in range(2):
            place = pl.ds(2 * i + half, 1)
            value = local_ref[:, place, :].reshape(2, nodes) - out[2 * half : 2 * half + 2]
            out_ref[:, place, :] = value.reshape(2, 1, nodes)
        return carry

    lax.fori_loop(0, modes // 2, two_modes, 0, unroll=2)


def leaf_down(own, rows, here, beside, local, joint):
    whole = pl.BlockSpec(memory_space=VMEM)
    return pl.pallas_call(
        leaf_down_kernel,
        out_shape=jax.ShapeDtypeStruct(local.shape, F32),
        in_specs=[pl.BlockSpec(memory_space=SMEM)] + [whole] * 5,
        out_specs=whole,
        scratch_shapes=[VMEM(here.shape, F32)],
        compiler_params=pltpu.CompilerParams(vmem_limit_bytes=LARGE),
        name="leaf_down",
    )(own, rows, here, beside, local, joint)


def spread_kernel(groups, me_ref, *refs):
    azi, rest, out_ref = refs[:groups], refs[groups : 2 * groups], refs[2 * groups]
    rows, width = azi[0].shape
    for k in range(groups):
        span = pl.ds(pl.multiple_of(jnp.bitwise_xor(me_ref[0], k) * width, 128), width)
        out_ref[:rows, span] = rest[k][:rows, :].astype(F32)
        out_ref[rows : 2 * rows, span] = azi[k][...].astype(F32)
        out_ref[2 * rows :, span] = rest[k][rows:, :].astype(F32)


def spread(me, azi, rest):
    groups = len(azi)
    rows, width = azi[0].shape
    return pl.pallas_call(
        functools.partial(spread_kernel, groups),
        out_shape=jax.ShapeDtypeStruct((3 * rows, groups * width), F32),
        in_specs=[pl.BlockSpec(memory_space=SMEM)] + [pl.BlockSpec(memory_space=VMEM)] * (2 * groups),
        out_specs=pl.BlockSpec(memory_space=VMEM),
        compiler_params=pltpu.CompilerParams(vmem_limit_bytes=16 * 2**20),
        name="spread",
    )(me, *azi, *rest)


def fronts_kernel(rows_ref, inv_ref, cpl_ref, out_ref):
    modes, size, _ = inv_ref.shape
    out_ref[0] = inv_ref[...]
    select = one_hot(rows_ref).astype(F32).T.astype(BF16)
    for m in range(modes):
        out_ref[1, m] = dot(select, cpl_ref[m]).astype(BF16)


def fronts(rows, inverse, coupling):
    return pl.pallas_call(
        fronts_kernel,
        out_shape=jax.ShapeDtypeStruct((2,) + inverse.shape, BF16),
        in_specs=[pl.BlockSpec(memory_space=VMEM)] * 3,
        out_specs=pl.BlockSpec(memory_space=VMEM),
        compiler_params=pltpu.CompilerParams(vmem_limit_bytes=SMALL),
        name="fronts",
    )(rows, inverse, coupling)


def apply_rows(x, matrix):
    modes, size, _ = matrix.shape
    wide = dot(x, matrix.reshape(modes * size, size), NT)
    row = lax.broadcasted_iota(jnp.int32, x.shape, 0) % modes
    total = jnp.zeros(x.shape, F32)
    for m in range(modes):
        total += jnp.where(row == m, wide[:, m * size : (m + 1) * size], 0.0)
    return total


def apply_columns(x, matrix):
    modes, size, _ = matrix.shape
    row = lax.broadcasted_iota(jnp.int32, x.shape, 0) % modes
    x = x.astype(F32)
    wide = jnp.concatenate([jnp.where(row == m, x, 0.0).astype(BF16) for m in range(modes)], axis=1)
    return dot(wide, matrix.reshape(modes * size, size))


def flat(ref):
    return ref[...].reshape(ref.shape[0] * ref.shape[1], ref.shape[2])


def rise_kernel(one_ref, two_ref, source_ref, front_ref, reduced_ref, outgoing_ref):
    g = (flat(source_ref) - (flat(one_ref) + flat(two_ref))).astype(BF16)
    reduced = apply_rows(g, front_ref[0]).astype(BF16)
    reduced_ref[...] = reduced.astype(F32).reshape(reduced_ref.shape)
    outgoing_ref[...] = apply_rows(reduced, front_ref[1]).reshape(outgoing_ref.shape)


def small_call(kernel, name, outs, args, scalars=0):
    return pl.pallas_call(
        kernel,
        out_shape=outs,
        in_specs=[pl.BlockSpec(memory_space=SMEM)] * scalars
        + [pl.BlockSpec(memory_space=VMEM)] * (len(args) - scalars),
        out_specs=[pl.BlockSpec(memory_space=VMEM)] * len(outs),
        compiler_params=pltpu.CompilerParams(vmem_limit_bytes=SMALL),
        name=name,
    )(*args)


def crown_kernel(high_ref, one_ref, two_ref, reduced_ref, front_ref, fa_ref, sa_ref, fb_ref, sb_ref, x_ref, x16_ref, far_ref):
    def solve(f_mid, s_mid, f_top, s_top, send_mid):
        g = (flat(s_mid) - (flat(one_ref) + flat(two_ref))).astype(BF16)
        mid = apply_rows(g, f_mid[0]).astype(BF16)
        g = (flat(s_top) - apply_rows(mid, f_mid[1])).astype(BF16)
        top = apply_columns(apply_rows(g, f_top[0]).astype(BF16), f_top[0])
        residue = mid.astype(F32) - apply_columns(top.astype(BF16), f_mid[1])
        x_mid = apply_columns(residue.astype(BF16), f_mid[0])
        far_ref[...] = (x_mid if send_mid else top).reshape(far_ref.shape)
        residue = flat(reduced_ref) - apply_columns(x_mid.astype(BF16), front_ref[1])
        x = apply_columns(residue.astype(BF16), front_ref[0])
        x_ref[...] = x.reshape(x_ref.shape)
        x16_ref[...] = x.astype(BF16).reshape(x_ref.shape)

    @pl.when(high_ref[0] == 0)
    def _():
        solve(fa_ref, sa_ref, fb_ref, sb_ref, False)

    @pl.when(high_ref[0] != 0)
    def _():
        solve(fb_ref, sb_ref, fa_ref, sa_ref, True)


def sink_kernel(one_ref, two_ref, reduced_ref, front_ref, x_ref, x16_ref):
    above = (flat(one_ref).astype(F32) + flat(two_ref).astype(F32)).astype(BF16)
    residue = flat(reduced_ref) - apply_columns(above, front_ref[1])
    x = apply_columns(residue.astype(BF16), front_ref[0])
    x_ref[...] = x.reshape(x_ref.shape)
    x16_ref[...] = x.astype(BF16).reshape(x_ref.shape)


def level_of(q, levels):
    return levels + 1 if q == 0 else (q & -q).bit_length()


def choose_kernel(level_ref, *refs):
    for at, ref in enumerate(refs[:-1]):

        @pl.when(level_ref[0] == at)
        def _(ref=ref):
            refs[-1][...] = ref[...]


def shards(
    velocity,
    magnetic,
    leaf_inverse,
    leaf_coupling,
    separator_inverse,
    separator_coupling,
    separator_source,
    front_rows,
):
    groups = lax.axis_size("mode")
    partitions = lax.axis_size("mesh")
    levels = partitions.bit_length() - 1
    modes, nodes = velocity.shape[2], velocity.shape[3]
    here = lax.axis_index("mode")
    me = here.reshape(1).astype(jnp.int32)
    position = lax.axis_index("mesh")
    exchange = [[(g, g ^ k) for g in range(groups)] for k in range(groups)]
    low, mid, high = partitions // 4, partitions // 2, 3 * partitions // 4

    def swap(pieces):
        return [pieces[0]] + [
            lax.ppermute(pieces[k], "mode", exchange[k]) for k in range(1, groups)
        ]

    def hop(value, pairs):
        return lax.ppermute(value, "mesh", pairs)

    packed = pack(me, velocity.reshape(6 * modes, nodes), magnetic.reshape(6 * modes, nodes), groups)
    spread_in = swap(packed)
    fwd, bwd = tables(me, groups, modes)
    rows_leaf, rows_front = front_rows[0, 0:1], front_rows[0, 1:2]
    front = fronts(rows_front, separator_inverse, separator_coupling)
    to_a, to_b = [(mid, low), (0, high)], [(mid, high), (0, low)]
    front_a, front_b = hop(front, to_a), hop(front, to_b)
    source_a, source_b = hop(separator_source, to_a), hop(separator_source, to_b)
    square, joint = compose(leaf_inverse, leaf_coupling)
    azi, rest = transform(fwd, bwd, spread_in)
    azi = swap(azi)
    rest = swap(rest)
    source, update = leaf_up(me, rows_leaf, magnetic, azi, joint)
    local = leaf_local(source, square)
    nonlinear = spread(me, azi, rest).reshape(3, 2, modes, nodes)

    of_level = [[q for q in range(partitions) if level_of(q, levels) == h] for h in range(levels + 2)]
    wide = jax.ShapeDtypeStruct(separator_source.shape, F32)
    half = jax.ShapeDtypeStruct(separator_source.shape, BF16)
    reduced = [None] * (levels + 1)
    one, two = update, hop(update, [(q - 1, q) for q in of_level[1]])
    for height in range(1, levels):
        if height > 1:
            gap = 2 ** (height - 2)
            one = hop(outgoing, [(q - gap, q) for q in of_level[height]])
            two = hop(outgoing, [(q + gap, q) for q in of_level[height]])
        reduced[height], outgoing = small_call(
            rise_kernel, "rise", [wide, wide], [one, two, separator_source, front]
        )
    other = hop(outgoing, [(low, high), (high, low)])
    is_high = (position == high).astype(jnp.int32).reshape(1)
    x, x16, far = small_call(
        crown_kernel,
        "crown",
        [wide, half, wide],
        [is_high, outgoing, other, reduced[levels - 1], front, front_a, source_a, front_b, source_b],
        scalars=1,
    )
    answers = [(levels - 1, x)]
    for height in range(levels - 2, 0, -1):
        gap = 2 ** (height - 1)
        one = hop(x16, [(q, q - gap) for q in of_level[height + 1]])
        two = hop(x16, [(q, q + gap) for q in of_level[height + 1]])
        x, x16 = small_call(sink_kernel, "sink", [wide, half], [one, two, reduced[height], front])
        answers.append((height, x))
    far = hop(far, [(low, 0), (high, mid)])
    beside = hop(x16, [(q, q - 1) for q in of_level[1]])
    level_here = sum((position % 2**t == 0).astype(jnp.int32) for t in range(1, levels + 1)) + 1
    own = (level_here == 1).astype(jnp.int32).reshape(1)
    azimuthal = leaf_down(own, rows_leaf, x16, beside, local, joint)
    answers.reverse()
    place = (jnp.minimum(level_here, levels) - 1).reshape(1)
    (solution,) = small_call(
        choose_kernel, "choose", [wide], [place] + [x for _, x in answers] + [far], scalars=1
    )
    return (nonlinear, azimuthal, solution)


def solution(mesh):
    in_specs = (
        P(None, None, "mode", "mesh"),
        P(None, None, "mode", "mesh"),
        P("mode", "mesh", None, None),
        P("mode", None, "mesh"),
        P("mode", "mesh", None),
        P("mode", "mesh", None),
        P(None, "mode", "mesh"),
        P("mesh", None, None),
    )
    out_specs = (P(None, None, "mode", "mesh"), P(None, "mode", "mesh"), P(None, "mode", "mesh"))
    return jax.shard_map(shards, mesh=mesh, in_specs=in_specs, out_specs=out_specs, check_vma=False)
```

```python
import functools

import jax
import jax.numpy as jnp
from jax import lax
from jax.experimental import pallas as pl
from jax.experimental.pallas import tpu as pltpu
from jax.sharding import PartitionSpec as P


NPHI = 192
DT_STEP = 0.5
VMEM = pltpu.VMEM
BF16 = jnp.bfloat16
F32 = jnp.float32
NT = (((1,), (1,)), ((), ()))
NN = (((1,), (0,)), ((), ()))
SMALL = 8 * 2**20
LARGE = 8 * 2**20
COMPOSE = 8 * 2**20


def stay(value):
    return pltpu.with_memory_space_constraint(value, pltpu.HBM)


def dot(a, b, dims=NN, precision=None):
    return lax.dot_general(a, b, dims, precision=precision, preferred_element_type=F32)


def tables_kernel(modes, fwd_ref, bwd_ref):
    def phase(shape, angle_axis):
        angle = lax.broadcasted_iota(jnp.int32, shape, angle_axis)
        at = lax.broadcasted_iota(jnp.int32, shape, 1 - angle_axis)
        step, kind, mode = at // (2 * modes), (at // modes) % 2, at % modes
        order = jnp.bitwise_xor(step, lax.axis_index("mode")) * modes + mode
        turn = (angle * order).astype(F32)
        turn = turn - NPHI * jnp.floor((turn + 0.5) * (1.0 / NPHI))
        return turn * (2.0 * jnp.pi / NPHI), kind, order

    at, kind, _ = phase(fwd_ref.shape, 0)
    fwd_ref[...] = jnp.where(kind == 0, jnp.cos(at), jnp.sin(at)).astype(BF16)
    at, kind, order = phase(bwd_ref.shape, 1)
    weight = jnp.where(order == 0, 1.0, 2.0) / NPHI
    bwd_ref[...] = (jnp.where(kind == 0, jnp.cos(at), jnp.sin(at)) * weight).astype(BF16)


def tables(groups, modes):
    rows = groups * 2 * modes
    return pl.pallas_call(
        functools.partial(tables_kernel, modes),
        out_shape=[jax.ShapeDtypeStruct((NPHI, rows), BF16), jax.ShapeDtypeStruct((rows, NPHI), BF16)],
        out_specs=[pl.BlockSpec(memory_space=VMEM)] * 2,
        compiler_params=pltpu.CompilerParams(vmem_limit_bytes=SMALL),
        name="tables",
    )()


def pack_kernel(groups, v_hbm, b_hbm, *refs):
    outs, held, sems = refs[:groups], refs[groups], refs[groups + 1]
    rows, width = v_hbm.shape[0], outs[0].shape[1]

    def copy(field, k):
        span = pl.ds(pl.multiple_of((lax.axis_index("mode") ^ k) * width, 128), width)
        source = (v_hbm, b_hbm)[field].at[:, span]
        return pltpu.make_async_copy(source, held.at[k, field], sems.at[k, field])

    order = list(range(1, groups)) + [0]
    for k in order:
        for field in range(2):
            copy(field, k).start()
    for k in order:
        for field in range(2):
            copy(field, k).wait()
            outs[k][field * rows : (field + 1) * rows, :] = held[k, field].astype(BF16)


def pack(velocity, magnetic, groups):
    rows, nodes = velocity.shape
    width = nodes // groups
    return pl.pallas_call(
        functools.partial(pack_kernel, groups),
        out_shape=[jax.ShapeDtypeStruct((2 * rows, width), BF16)] * groups,
        in_specs=[pl.BlockSpec(memory_space=pltpu.HBM)] * 2,
        out_specs=[pl.BlockSpec(memory_space=VMEM)] * groups,
        scratch_shapes=[VMEM((groups, 2, rows, width), F32), pltpu.SemaphoreType.DMA((groups, 2))],
        compiler_params=pltpu.CompilerParams(vmem_limit_bytes=SMALL),
        name="pack",
    )(velocity, magnetic)


def transform_kernel(groups, fwd_ref, bwd_ref, *refs):
    ins, azi, rest = refs[:groups], refs[groups : 2 * groups], refs[2 * groups :]
    rows = ins[0].shape[0] // 6
    fwd, bwd = fwd_ref[...], bwd_ref[...]
    phys = []
    for field in range(6):
        coef = jnp.concatenate([r[field * rows : (field + 1) * rows, :] for r in ins], axis=0)
        phys.append(dot(fwd, coef))
    v, b = phys[:3], phys[3:]
    for c in range(3):
        p, q = (c + 1) % 3, (c + 2) % 3
        crossed = (v[p] * b[q] - v[q] * b[p]).astype(BF16)
        terms = dot(bwd, crossed).astype(BF16)
        for k in range(groups):
            block = terms[k * rows : (k + 1) * rows, :]
            if c == 1:
                azi[k][...] = block
            else:
                at = 0 if c == 0 else rows
                rest[k][at : at + rows, :] = block


def transform(fwd, bwd, pieces):
    groups = len(pieces)
    rows, width = pieces[0].shape
    rows = rows // 6
    out = pl.pallas_call(
        functools.partial(transform_kernel, groups),
        out_shape=[jax.ShapeDtypeStruct((rows, width), BF16)] * groups
        + [jax.ShapeDtypeStruct((2 * rows, width), BF16)] * groups,
        in_specs=[pl.BlockSpec(memory_space=VMEM)] * (2 + groups),
        out_specs=[pl.BlockSpec(memory_space=VMEM)] * (2 * groups),
        compiler_params=pltpu.CompilerParams(vmem_limit_bytes=24 * 2**20),
        name="transform",
    )(fwd, bwd, *pieces)
    return out[:groups], out[groups:]


def one_hot(rows_ref, which):
    n = rows_ref.shape[2]
    return lax.broadcasted_iota(jnp.int32, (n, n), 0) == rows_ref[0, which : which + 1, :]


def compose_kernel(inv_hbm, cpl_hbm, square_ref, joint_ref, inv_v, cpl_v, sems):
    modes, front, _ = joint_ref.shape
    blocks, size = inv_v.shape[1], inv_v.shape[2]
    depth = inv_v.shape[0]
    zero = jnp.zeros((size, size), BF16)

    def copies(m):
        slot = m % depth
        return (
            pltpu.make_async_copy(inv_hbm.at[m], inv_v.at[slot], sems.at[0, slot]),
            pltpu.make_async_copy(cpl_hbm.at[m], cpl_v.at[slot], sems.at[1, slot]),
        )

    for m in range(depth):
        for copy in copies(m):
            copy.start()

    def one_mode(m, carry):
        slot = m % depth
        for copy in copies(m):
            copy.wait()
        for b in range(0, blocks, 2):
            first, second = inv_v[slot, b], inv_v[slot, b + 1]
            weights = jnp.concatenate(
                [jnp.concatenate([first, zero], axis=1), jnp.concatenate([zero, second], axis=1)],
                axis=0,
            )
            span = slice(b * size, (b + 2) * size)
            rows = jnp.concatenate(
                [cpl_v[slot, :, span], jnp.concatenate([first.T, second.T], axis=1)], axis=0
            )
            out = dot(rows, weights).astype(BF16)
            joint_ref[m, :, span] = out[:front]
            square_ref[m, b] = out[front:, :size]
            square_ref[m, b + 1] = out[front:, size:]

        @pl.when(m + depth < modes)
        def _():
            for copy in copies(m + depth):
                copy.start()

        return carry

    lax.fori_loop(0, modes, one_mode, 0)


def compose(inverse, coupling, depth=4):
    modes, blocks, size, _ = inverse.shape
    front, nodes = coupling.shape[1:]
    return pl.pallas_call(
        compose_kernel,
        out_shape=[
            jax.ShapeDtypeStruct(inverse.shape, BF16),
            jax.ShapeDtypeStruct(coupling.shape, BF16),
        ],
        in_specs=[pl.BlockSpec(memory_space=pltpu.HBM)] * 2,
        out_specs=[pl.BlockSpec(memory_space=VMEM)] * 2,
        scratch_shapes=[
            VMEM((depth, blocks, size, size), BF16),
            VMEM((depth, front, nodes), BF16),
            pltpu.SemaphoreType.DMA((2, depth)),
        ],
        compiler_params=pltpu.CompilerParams(vmem_limit_bytes=COMPOSE),
        cost_estimate=pl.CostEstimate(
            flops=4 * modes * nodes * size * (front + size),
            bytes_accessed=4 * (inverse.size + coupling.size),
            transcendentals=0,
        ),
        name="compose",
    )(inverse, coupling)


def leaf_up_kernel(groups, rows_ref, mag_hbm, joint_ref, *refs):
    pieces = refs[:groups]
    source_ref, update_ref, turned_v, mag_v, sem = refs[groups:]
    copy = pltpu.make_async_copy(mag_hbm.at[1], mag_v, sem)
    copy.start()
    copy.wait()
    modes, front, nodes = joint_ref.shape
    width = nodes // groups
    for k in range(groups):
        span = pl.ds(pl.multiple_of((lax.axis_index("mode") ^ k) * width, 128), width)
        for a in range(2):
            term = pieces[k][a * modes : (a + 1) * modes, :].astype(F32)
            source_ref[a, :, span] = mag_v[a, :, span] + DT_STEP * term
    turned_v[...] = source_ref[...].reshape(2 * modes, nodes).T.astype(BF16)
    turned = turned_v[...]
    lane = lax.broadcasted_iota(jnp.int32, (front, 2 * modes), 1) % modes

    def one_mode(m, total):
        return total + jnp.where(lane == m, dot(joint_ref[m], turned), 0.0)

    total = lax.fori_loop(0, modes, one_mode, jnp.zeros((front, 2 * modes), F32), unroll=2)
    select = one_hot(rows_ref, 0).astype(F32)
    update_ref[...] = dot(total.T, select, precision=lax.Precision.HIGHEST).reshape(update_ref.shape)


def leaf_up(rows, magnetic, pieces, joint):
    modes, front, nodes = joint.shape
    groups = len(pieces)
    whole = pl.BlockSpec(memory_space=VMEM)
    return pl.pallas_call(
        functools.partial(leaf_up_kernel, groups),
        out_shape=[
            jax.ShapeDtypeStruct((2, modes, nodes), F32),
            jax.ShapeDtypeStruct((2, modes, front), F32),
        ],
        in_specs=[
            whole,
            pl.BlockSpec(memory_space=pltpu.HBM),
        ]
        + [whole] * (1 + groups),
        out_specs=[whole] * 2,
        scratch_shapes=[
            VMEM((nodes, 2 * modes), BF16),
            VMEM((2, modes, nodes), F32),
            pltpu.SemaphoreType.DMA(()),
        ],
        compiler_params=pltpu.CompilerParams(vmem_limit_bytes=LARGE),
        cost_estimate=pl.CostEstimate(
            flops=128 * modes * nodes * front, bytes_accessed=2 * joint.size, transcendentals=0
        ),
        name="leaf_up",
    )(rows, magnetic, joint, *pieces)


def leaf_local_kernel(source_ref, square_ref, out_ref):
    modes, blocks, size, _ = square_ref.shape
    nodes = blocks * size
    zero = jnp.zeros((2, size), BF16)

    def one_mode(m, carry):
        source = source_ref[:, pl.ds(m, 1), :].reshape(2, nodes).astype(BF16)
        parts = []
        for b in range(0, blocks, 2):
            one = source[:, b * size : (b + 1) * size]
            two = source[:, (b + 1) * size : (b + 2) * size]
            left = jnp.concatenate(
                [jnp.concatenate([one, zero], axis=1), jnp.concatenate([zero, two], axis=1)], axis=0
            )
            pair = dot(left, square_ref[m, b : b + 2].reshape(2 * size, size))
            parts += [pair[:2], pair[2:]]
        out_ref[:, pl.ds(m, 1), :] = jnp.concatenate(parts, axis=1).reshape(2, 1, nodes)
        return carry

    lax.fori_loop(0, modes, one_mode, 0, unroll=2)


def leaf_local(source, square):
    whole = pl.BlockSpec(memory_space=VMEM)
    return pl.pallas_call(
        leaf_local_kernel,
        out_shape=jax.ShapeDtypeStruct(source.shape, F32),
        in_specs=[whole] * 2,
        out_specs=whole,
        compiler_params=pltpu.CompilerParams(vmem_limit_bytes=LARGE),
        cost_estimate=pl.CostEstimate(
            flops=128 * square.size, bytes_accessed=2 * square.size, transcendentals=0
        ),
        name="leaf_local",
    )(source, square)


def leaf_down_kernel(rows_ref, here_ref, beside_ref, local_ref, joint_ref, out_ref, x_v):
    modes, front, nodes = joint_ref.shape
    select = one_hot(rows_ref, 0).astype(F32).astype(BF16)
    above = jnp.where(lax.axis_index("mesh") % 2 == 1, here_ref[...].astype(F32), beside_ref[...].astype(F32))
    x_v[...] = dot(above.reshape(2 * modes, front).astype(BF16), select, NT).reshape(2, modes, front)
    zero = jnp.zeros((2, front), F32)

    def two_modes(i, carry):
        one = x_v[:, pl.ds(2 * i, 1), :].reshape(2, front)
        two = x_v[:, pl.ds(2 * i + 1, 1), :].reshape(2, front)
        left = jnp.concatenate(
            [jnp.concatenate([one, zero], axis=1), jnp.concatenate([zero, two], axis=1)], axis=0
        ).astype(BF16)
        out = dot(left, joint_ref[pl.ds(2 * i, 2)].reshape(2 * front, nodes))
        for half in range(2):
            place = pl.ds(2 * i + half, 1)
            value = local_ref[:, place, :].reshape(2, nodes) - out[2 * half : 2 * half + 2]
            out_ref[:, place, :] = value.reshape(2, 1, nodes)
        return carry

    lax.fori_loop(0, modes // 2, two_modes, 0, unroll=2)


def leaf_down(rows, here, beside, local, joint):
    whole = pl.BlockSpec(memory_space=VMEM)
    return pl.pallas_call(
        leaf_down_kernel,
        out_shape=jax.ShapeDtypeStruct(local.shape, F32),
        in_specs=[whole] * 5,
        out_specs=whole,
        scratch_shapes=[VMEM(here.shape, F32)],
        compiler_params=pltpu.CompilerParams(vmem_limit_bytes=LARGE),
        name="leaf_down",
    )(rows, here, beside, local, joint)


def spread_kernel(groups, *refs):
    azi, rest, out_ref = refs[:groups], refs[groups : 2 * groups], refs[2 * groups]
    rows, width = azi[0].shape
    for k in range(groups):
        span = pl.ds(pl.multiple_of((lax.axis_index("mode") ^ k) * width, 128), width)
        out_ref[:rows, span] = rest[k][:rows, :].astype(F32)
        out_ref[rows : 2 * rows, span] = azi[k][...].astype(F32)
        out_ref[2 * rows :, span] = rest[k][rows:, :].astype(F32)


def spread(azi, rest):
    groups = len(azi)
    rows, width = azi[0].shape
    return pl.pallas_call(
        functools.partial(spread_kernel, groups),
        out_shape=jax.ShapeDtypeStruct((3 * rows, groups * width), F32),
        in_specs=[pl.BlockSpec(memory_space=VMEM)] * (2 * groups),
        out_specs=pl.BlockSpec(memory_space=VMEM),
        compiler_params=pltpu.CompilerParams(vmem_limit_bytes=16 * 2**20),
        name="spread",
    )(*azi, *rest)


def fronts_kernel(rows_ref, inv_ref, cpl_ref, source_ref, out_ref):
    modes, size, _ = inv_ref.shape
    half = modes * size
    out_ref[:half, :] = inv_ref[...].reshape(half, size)
    select = one_hot(rows_ref, 1).astype(F32).T.astype(BF16)
    for m in range(modes):
        at = half + m * size
        out_ref[at : at + size, :] = dot(select, cpl_ref[m]).astype(BF16)
    rest = flat(source_ref)
    for part in range(3):
        at = 2 * half + part * rest.shape[0]
        term = rest.astype(BF16)
        out_ref[at : at + rest.shape[0], :] = term
        rest = rest - term.astype(F32)


def fronts(rows, inverse, coupling, source):
    modes, size, _ = inverse.shape
    total = 2 * modes * size + 3 * 2 * modes
    return pl.pallas_call(
        fronts_kernel,
        out_shape=jax.ShapeDtypeStruct((total, size), BF16),
        in_specs=[pl.BlockSpec(memory_space=VMEM)] * 4,
        out_specs=pl.BlockSpec(memory_space=VMEM),
        compiler_params=pltpu.CompilerParams(vmem_limit_bytes=SMALL),
        name="fronts",
    )(rows, inverse, coupling, source)


class Front:
    def __init__(self, ref, like):
        count, modes, size = like.shape
        self.ref, self.modes, self.size, self.rows = ref, modes, size, count * modes

    def __getitem__(self, which):
        half = self.modes * self.size
        return self.ref[which * half : (which + 1) * half, :].reshape(self.modes, self.size, self.size)

    def source(self):
        at = 2 * self.modes * self.size
        parts = [self.ref[at + p * self.rows : at + (p + 1) * self.rows, :].astype(F32) for p in range(3)]
        return parts[0] + parts[1] + parts[2]


def apply_rows(x, matrix):
    modes, size, _ = matrix.shape
    wide = dot(x, matrix.reshape(modes * size, size), NT)
    row = lax.broadcasted_iota(jnp.int32, x.shape, 0) % modes
    total = jnp.zeros(x.shape, F32)
    for m in range(modes):
        total += jnp.where(row == m, wide[:, m * size : (m + 1) * size], 0.0)
    return total


def apply_columns(x, matrix):
    modes, size, _ = matrix.shape
    row = lax.broadcasted_iota(jnp.int32, x.shape, 0) % modes
    x = x.astype(F32)
    wide = jnp.concatenate([jnp.where(row == m, x, 0.0).astype(BF16) for m in range(modes)], axis=1)
    return dot(wide, matrix.reshape(modes * size, size))


def flat(ref):
    return ref[...].reshape(ref.shape[0] * ref.shape[1], ref.shape[2])


def rise_kernel(one_ref, two_ref, source_ref, front_ref, reduced_ref, outgoing_ref):
    front_ref = Front(front_ref, one_ref)
    g = (flat(source_ref) - (flat(one_ref) + flat(two_ref))).astype(BF16)
    reduced = apply_rows(g, front_ref[0]).astype(BF16)
    reduced_ref[...] = reduced.astype(F32).reshape(reduced_ref.shape)
    outgoing_ref[...] = apply_rows(reduced, front_ref[1]).reshape(outgoing_ref.shape)


def small_call(kernel, outs, args):
    return pl.pallas_call(
        kernel,
        out_shape=outs,
        in_specs=[pl.BlockSpec(memory_space=VMEM)] * len(args),
        out_specs=[pl.BlockSpec(memory_space=VMEM)] * len(outs),
        compiler_params=pltpu.CompilerParams(vmem_limit_bytes=SMALL),
    )(*args)


def crown_kernel(high, one_ref, two_ref, reduced_ref, front_ref, fa_ref, fb_ref, x_ref, x16_ref, far_ref):
    front_ref, front_a, front_b = (Front(ref, one_ref) for ref in (front_ref, fa_ref, fb_ref))

    def solve(f_mid, f_top, send_mid):
        g = (f_mid.source() - (flat(one_ref) + flat(two_ref))).astype(BF16)
        mid = apply_rows(g, f_mid[0]).astype(BF16)
        g = (f_top.source() - apply_rows(mid, f_mid[1])).astype(BF16)
        top = apply_columns(apply_rows(g, f_top[0]).astype(BF16), f_top[0])
        residue = mid.astype(F32) - apply_columns(top.astype(BF16), f_mid[1])
        x_mid = apply_columns(residue.astype(BF16), f_mid[0])
        far_ref[...] = (x_mid if send_mid else top).reshape(far_ref.shape)
        residue = flat(reduced_ref) - apply_columns(x_mid.astype(BF16), front_ref[1])
        x = apply_columns(residue.astype(BF16), front_ref[0])
        x_ref[...] = x.reshape(x_ref.shape)
        x16_ref[...] = x.astype(BF16).reshape(x_ref.shape)

    @pl.when(lax.axis_index("mesh") != high)
    def _():
        solve(front_a, front_b, False)

    @pl.when(lax.axis_index("mesh") == high)
    def _():
        solve(front_b, front_a, True)


def sink_kernel(one_ref, two_ref, reduced_ref, front_ref, x_ref, x16_ref):
    front_ref = Front(front_ref, one_ref)
    above = (flat(one_ref).astype(F32) + flat(two_ref).astype(F32)).astype(BF16)
    residue = flat(reduced_ref) - apply_columns(above, front_ref[1])
    x = apply_columns(residue.astype(BF16), front_ref[0])
    x_ref[...] = x.reshape(x_ref.shape)
    x16_ref[...] = x.astype(BF16).reshape(x_ref.shape)


def level_of(q, levels):
    return levels + 1 if q == 0 else (q & -q).bit_length()


def choose_kernel(*refs):
    position = lax.axis_index("mesh")
    last = len(refs) - 2
    for at, ref in enumerate(refs[:-1]):
        here = position % 2**at == 0
        if at < last:
            here &= position % 2 ** (at + 1) != 0

        @pl.when(here)
        def _(ref=ref):
            refs[-1][...] = ref[...]


def shards(
    velocity,
    magnetic,
    leaf_inverse,
    leaf_coupling,
    separator_inverse,
    separator_coupling,
    separator_source,
    front_rows,
):
    groups = lax.axis_size("mode")
    partitions = lax.axis_size("mesh")
    levels = partitions.bit_length() - 1
    modes, nodes = velocity.shape[2], velocity.shape[3]
    exchange = [[(g, g ^ k) for g in range(groups)] for k in range(groups)]
    low, mid, high = partitions // 4, partitions // 2, 3 * partitions // 4

    def swap(pieces):
        out = [pieces[0]]
        for k in range(1, groups):
            out.append(lax.ppermute(pieces[k], "mode", exchange[k]))
        return out

    def hop(value, pairs):
        return lax.ppermute(value, "mesh", pairs)

    packed = pack(stay(velocity.reshape(6 * modes, nodes)), stay(magnetic.reshape(6 * modes, nodes)), groups)
    spread_in = swap(packed)
    fwd, bwd = tables(groups, modes)
    front = fronts(front_rows, separator_inverse, separator_coupling, separator_source)
    front_a = hop(front, [(mid, low), (0, high)])
    front_b = hop(front, [(mid, high), (0, low)])
    square, joint = compose(stay(leaf_inverse), stay(leaf_coupling))
    azi, rest = transform(fwd, bwd, spread_in)
    azi = swap(azi)
    rest = swap(rest)
    source, update = leaf_up(front_rows, stay(magnetic), azi, joint)
    local = leaf_local(source, square)
    nonlinear = spread(azi, rest).reshape(3, 2, modes, nodes)

    of_level = [[q for q in range(partitions) if level_of(q, levels) == h] for h in range(levels + 2)]
    wide = jax.ShapeDtypeStruct(separator_source.shape, F32)
    half = jax.ShapeDtypeStruct(separator_source.shape, BF16)
    reduced = [None] * (levels + 1)
    one, two = update, hop(update, [(q - 1, q) for q in of_level[1]])
    for height in range(1, levels):
        if height > 1:
            gap = 2 ** (height - 2)
            one = hop(outgoing, [(q - gap, q) for q in of_level[height]])
            two = hop(outgoing, [(q + gap, q) for q in of_level[height]])
        reduced[height], outgoing = small_call(rise_kernel, [wide, wide], [one, two, separator_source, front])
    other = hop(outgoing, [(low, high), (high, low)])
    x, x16, far = small_call(
        functools.partial(crown_kernel, high),
        [wide, half, wide],
        [outgoing, other, reduced[levels - 1], front, front_a, front_b],
    )
    answers = [(levels - 1, x)]
    for height in range(levels - 2, 0, -1):
        gap = 2 ** (height - 1)
        one = hop(x16, [(q, q - gap) for q in of_level[height + 1]])
        two = hop(x16, [(q, q + gap) for q in of_level[height + 1]])
        x, x16 = small_call(sink_kernel, [wide, half], [one, two, reduced[height], front])
        answers.append((height, x))
    far = hop(far, [(low, 0), (high, mid)])
    beside = hop(x16, [(q, q - 1) for q in of_level[1]])
    azimuthal = leaf_down(front_rows, x16, beside, local, joint)
    answers.reverse()
    (solution,) = small_call(choose_kernel, [wide], [x for _, x in answers] + [far])
    return (nonlinear, azimuthal, solution)


def solution(mesh):
    in_specs = (
        P(None, None, "mode", "mesh"),
        P(None, None, "mode", "mesh"),
        P("mode", "mesh", None, None),
        P("mode", None, "mesh"),
        P("mode", "mesh", None),
        P("mode", "mesh", None),
        P(None, "mode", "mesh"),
        P("mesh", None, None),
    )
    out_specs = (P(None, None, "mode", "mesh"), P(None, "mode", "mesh"), P(None, "mode", "mesh"))


    return jax.shard_map(shards, mesh=mesh, in_specs=in_specs, out_specs=out_specs, check_vma=False)
```

```python
import functools

import jax
import jax.numpy as jnp
from jax import lax
from jax.experimental import pallas as pl
from jax.experimental.pallas import tpu as pltpu
from jax.sharding import PartitionSpec as P


NPHI = 192
DT_STEP = 0.5
VMEM = pltpu.VMEM
BF16 = jnp.bfloat16
F32 = jnp.float32
NT = (((1,), (1,)), ((), ()))
NN = (((1,), (0,)), ((), ()))
SMALL = 8 * 2**20
LARGE = 8 * 2**20
COMPOSE = 8 * 2**20


def stay(value):
    return pltpu.with_memory_space_constraint(value, pltpu.HBM)


def dot(a, b, dims=NN, precision=None):
    return lax.dot_general(a, b, dims, precision=precision, preferred_element_type=F32)


def tables_kernel(modes, fwd_ref, bwd_ref):
    def phase(shape, angle_axis):
        angle = lax.broadcasted_iota(jnp.int32, shape, angle_axis)
        at = lax.broadcasted_iota(jnp.int32, shape, 1 - angle_axis)
        step, kind, mode = at // (2 * modes), (at // modes) % 2, at % modes
        order = jnp.bitwise_xor(step, lax.axis_index("mode")) * modes + mode
        turn = (angle * order).astype(F32)
        turn = turn - NPHI * jnp.floor((turn + 0.5) * (1.0 / NPHI))
        return turn * (2.0 * jnp.pi / NPHI), kind, order

    at, kind, _ = phase(fwd_ref.shape, 0)
    fwd_ref[...] = jnp.where(kind == 0, jnp.cos(at), jnp.sin(at)).astype(BF16)
    at, kind, order = phase(bwd_ref.shape, 1)
    weight = jnp.where(order == 0, 1.0, 2.0) / NPHI
    bwd_ref[...] = (jnp.where(kind == 0, jnp.cos(at), jnp.sin(at)) * weight).astype(BF16)


def tables(groups, modes):
    rows = groups * 2 * modes
    return pl.pallas_call(
        functools.partial(tables_kernel, modes),
        out_shape=[jax.ShapeDtypeStruct((NPHI, rows), BF16), jax.ShapeDtypeStruct((rows, NPHI), BF16)],
        out_specs=[pl.BlockSpec(memory_space=VMEM)] * 2,
        compiler_params=pltpu.CompilerParams(vmem_limit_bytes=SMALL),
        name="tables",
    )()


def pack_kernel(groups, v_hbm, b_hbm, *refs):
    outs, azi_ref, held, sems = refs[:groups], refs[groups], refs[groups + 1], refs[groups + 2]
    rows, width = v_hbm.shape[0], outs[0].shape[1]
    part = rows // 3

    def copy(field, k):
        span = pl.ds(pl.multiple_of((lax.axis_index("mode") ^ k) * width, 128), width)
        source = (v_hbm, b_hbm)[field].at[:, span]
        return pltpu.make_async_copy(source, held.at[k, field], sems.at[k, field])

    order = list(range(1, groups)) + [0]
    for k in order:
        for field in range(2):
            copy(field, k).start()
    for k in order:
        for field in range(2):
            copy(field, k).wait()
            outs[k][field * rows : (field + 1) * rows, :] = held[k, field].astype(BF16)
    for k in order:
        span = pl.ds(pl.multiple_of((lax.axis_index("mode") ^ k) * width, 128), width)
        azi_ref[:, span] = held[k, 1, part : 2 * part]


def pack(velocity, magnetic, groups):
    rows, nodes = velocity.shape
    width = nodes // groups
    return pl.pallas_call(
        functools.partial(pack_kernel, groups),
        out_shape=[jax.ShapeDtypeStruct((2 * rows, width), BF16)] * groups
        + [jax.ShapeDtypeStruct((rows // 3, nodes), F32)],
        in_specs=[pl.BlockSpec(memory_space=pltpu.HBM)] * 2,
        out_specs=[pl.BlockSpec(memory_space=VMEM)] * (groups + 1),
        scratch_shapes=[VMEM((groups, 2, rows, width), F32), pltpu.SemaphoreType.DMA((groups, 2))],
        compiler_params=pltpu.CompilerParams(vmem_limit_bytes=SMALL),
        name="pack",
    )(velocity, magnetic)


def transform_kernel(groups, fwd_ref, bwd_ref, *refs):
    ins, azi, rest = refs[:groups], refs[groups : 2 * groups], refs[2 * groups :]
    rows = ins[0].shape[0] // 6
    fwd, bwd = fwd_ref[...], bwd_ref[...]
    phys = []
    for field in range(6):
        coef = jnp.concatenate([r[field * rows : (field + 1) * rows, :] for r in ins], axis=0)
        phys.append(dot(fwd, coef))
    v, b = phys[:3], phys[3:]
    for c in range(3):
        p, q = (c + 1) % 3, (c + 2) % 3
        crossed = (v[p] * b[q] - v[q] * b[p]).astype(BF16)
        terms = dot(bwd, crossed).astype(BF16)
        for k in range(groups):
            block = terms[k * rows : (k + 1) * rows, :]
            if c == 1:
                azi[k][...] = block
            else:
                at = 0 if c == 0 else rows
                rest[k][at : at + rows, :] = block


def transform(fwd, bwd, pieces):
    groups = len(pieces)
    rows, width = pieces[0].shape
    rows = rows // 6
    out = pl.pallas_call(
        functools.partial(transform_kernel, groups),
        out_shape=[jax.ShapeDtypeStruct((rows, width), BF16)] * groups
        + [jax.ShapeDtypeStruct((2 * rows, width), BF16)] * groups,
        in_specs=[pl.BlockSpec(memory_space=VMEM)] * (2 + groups),
        out_specs=[pl.BlockSpec(memory_space=VMEM)] * (2 * groups),
        compiler_params=pltpu.CompilerParams(vmem_limit_bytes=24 * 2**20),
        name="transform",
    )(fwd, bwd, *pieces)
    return out[:groups], out[groups:]


def one_hot(rows_ref, which):
    n = rows_ref.shape[2]
    return lax.broadcasted_iota(jnp.int32, (n, n), 0) == rows_ref[0, which : which + 1, :]


def compose_kernel(inv_hbm, cpl_hbm, square_ref, joint_ref, inv_v, cpl_v, sems):
    modes, front, _ = joint_ref.shape
    blocks, size = inv_v.shape[1], inv_v.shape[2]
    depth = inv_v.shape[0]
    zero = jnp.zeros((size, size), BF16)

    def copies(m):
        slot = m % depth
        return (
            pltpu.make_async_copy(inv_hbm.at[m], inv_v.at[slot], sems.at[0, slot]),
            pltpu.make_async_copy(cpl_hbm.at[m], cpl_v.at[slot], sems.at[1, slot]),
        )

    for m in range(depth):
        for copy in copies(m):
            copy.start()

    def one_mode(m, carry):
        slot = m % depth
        for copy in copies(m):
            copy.wait()
        for b in range(0, blocks, 2):
            first, second = inv_v[slot, b], inv_v[slot, b + 1]
            weights = jnp.concatenate(
                [jnp.concatenate([first, zero], axis=1), jnp.concatenate([zero, second], axis=1)],
                axis=0,
            )
            span = slice(b * size, (b + 2) * size)
            rows = jnp.concatenate(
                [cpl_v[slot, :, span], jnp.concatenate([first.T, second.T], axis=1)], axis=0
            )
            out = dot(rows, weights).astype(BF16)
            joint_ref[m, :, span] = out[:front]
            square_ref[m, b] = out[front:, :size]
            square_ref[m, b + 1] = out[front:, size:]

        @pl.when(m + depth < modes)
        def _():
            for copy in copies(m + depth):
                copy.start()

        return carry

    lax.fori_loop(0, modes, one_mode, 0)


def compose(inverse, coupling, depth=4):
    modes, blocks, size, _ = inverse.shape
    front, nodes = coupling.shape[1:]
    return pl.pallas_call(
        compose_kernel,
        out_shape=[
            jax.ShapeDtypeStruct(inverse.shape, BF16),
            jax.ShapeDtypeStruct(coupling.shape, BF16),
        ],
        in_specs=[pl.BlockSpec(memory_space=pltpu.HBM)] * 2,
        out_specs=[pl.BlockSpec(memory_space=VMEM)] * 2,
        scratch_shapes=[
            VMEM((depth, blocks, size, size), BF16),
            VMEM((depth, front, nodes), BF16),
            pltpu.SemaphoreType.DMA((2, depth)),
        ],
        compiler_params=pltpu.CompilerParams(vmem_limit_bytes=COMPOSE),
        cost_estimate=pl.CostEstimate(
            flops=4 * modes * nodes * size * (front + size),
            bytes_accessed=4 * (inverse.size + coupling.size),
            transcendentals=0,
        ),
        name="compose",
    )(inverse, coupling)


def leaf_up_kernel(groups, rows_ref, mag_ref, joint_ref, *refs):
    pieces = refs[:groups]
    source_ref, update_ref, turned_v = refs[groups:]
    modes, front, nodes = joint_ref.shape
    width = nodes // groups
    for k in range(groups):
        at = pl.multiple_of((lax.axis_index("mode") ^ k) * width, 128)
        span = pl.ds(at, width)
        source = (mag_ref[:, span] + DT_STEP * pieces[k][...].astype(F32)).astype(BF16)
        source_ref[:, :, span] = source.astype(F32).reshape(2, modes, width)
        turned_v[pl.ds(at, width), :] = source.T
    turned = turned_v[...]
    lane = lax.broadcasted_iota(jnp.int32, (front, 2 * modes), 1) % modes

    def one_mode(m, total):
        return total + jnp.where(lane == m, dot(joint_ref[m], turned), 0.0)

    total = lax.fori_loop(0, modes, one_mode, jnp.zeros((front, 2 * modes), F32), unroll=4)
    select = one_hot(rows_ref, 0).astype(F32)
    update_ref[...] = dot(total.T, select, precision=lax.Precision.HIGHEST).reshape(update_ref.shape)


def leaf_up(rows, mag, pieces, joint):
    modes, front, nodes = joint.shape
    groups = len(pieces)
    whole = pl.BlockSpec(memory_space=VMEM)
    return pl.pallas_call(
        functools.partial(leaf_up_kernel, groups),
        out_shape=[
            jax.ShapeDtypeStruct((2, modes, nodes), F32),
            jax.ShapeDtypeStruct((2, modes, front), F32),
        ],
        in_specs=[whole] * (3 + groups),
        out_specs=[whole] * 2,
        scratch_shapes=[VMEM((nodes, 2 * modes), BF16)],
        compiler_params=pltpu.CompilerParams(vmem_limit_bytes=LARGE),
        cost_estimate=pl.CostEstimate(
            flops=128 * modes * nodes * front, bytes_accessed=2 * joint.size, transcendentals=0
        ),
        name="leaf_up",
    )(rows, mag, joint, *pieces)


def leaf_local_kernel(source_ref, square_ref, out_ref):
    modes, blocks, size, _ = square_ref.shape
    nodes = blocks * size
    zero = jnp.zeros((2, size), BF16)

    def one_mode(m, carry):
        source = source_ref[:, pl.ds(m, 1), :].reshape(2, nodes).astype(BF16)
        parts = []
        for b in range(0, blocks, 2):
            one = source[:, b * size : (b + 1) * size]
            two = source[:, (b + 1) * size : (b + 2) * size]
            left = jnp.concatenate(
                [jnp.concatenate([one, zero], axis=1), jnp.concatenate([zero, two], axis=1)], axis=0
            )
            pair = dot(left, square_ref[m, b : b + 2].reshape(2 * size, size))
            parts += [pair[:2], pair[2:]]
        out_ref[:, pl.ds(m, 1), :] = jnp.concatenate(parts, axis=1).reshape(2, 1, nodes)
        return carry

    lax.fori_loop(0, modes, one_mode, 0, unroll=2)


def leaf_local(source, square):
    whole = pl.BlockSpec(memory_space=VMEM)
    return pl.pallas_call(
        leaf_local_kernel,
        out_shape=jax.ShapeDtypeStruct(source.shape, F32),
        in_specs=[whole] * 2,
        out_specs=whole,
        compiler_params=pltpu.CompilerParams(vmem_limit_bytes=LARGE),
        cost_estimate=pl.CostEstimate(
            flops=128 * square.size, bytes_accessed=2 * square.size, transcendentals=0
        ),
        name="leaf_local",
    )(source, square)


def leaf_down_kernel(rows_ref, here_ref, beside_ref, local_ref, joint_ref, out_ref, x_v):
    modes, front, nodes = joint_ref.shape
    select = one_hot(rows_ref, 0).astype(F32).astype(BF16)
    above = jnp.where(lax.axis_index("mesh") % 2 == 1, here_ref[...].astype(F32), beside_ref[...].astype(F32))
    x_v[...] = dot(above.reshape(2 * modes, front).astype(BF16), select, NT).reshape(2, modes, front)
    zero = jnp.zeros((2, front), F32)

    def two_modes(i, carry):
        one = x_v[:, pl.ds(2 * i, 1), :].reshape(2, front)
        two = x_v[:, pl.ds(2 * i + 1, 1), :].reshape(2, front)
        left = jnp.concatenate(
            [jnp.concatenate([one, zero], axis=1), jnp.concatenate([zero, two], axis=1)], axis=0
        ).astype(BF16)
        out = dot(left, joint_ref[pl.ds(2 * i, 2)].reshape(2 * front, nodes))
        for half in range(2):
            place = pl.ds(2 * i + half, 1)
            value = local_ref[:, place, :].reshape(2, nodes) - out[2 * half : 2 * half + 2]
            out_ref[:, place, :] = value.reshape(2, 1, nodes)
        return carry

    lax.fori_loop(0, modes // 2, two_modes, 0, unroll=2)


def leaf_down(rows, here, beside, local, joint):
    whole = pl.BlockSpec(memory_space=VMEM)
    return pl.pallas_call(
        leaf_down_kernel,
        out_shape=jax.ShapeDtypeStruct(local.shape, F32),
        in_specs=[whole] * 5,
        out_specs=whole,
        scratch_shapes=[VMEM(here.shape, F32)],
        compiler_params=pltpu.CompilerParams(vmem_limit_bytes=LARGE),
        name="leaf_down",
    )(rows, here, beside, local, joint)


def spread_kernel(groups, *refs):
    azi, rest, out_ref = refs[:groups], refs[groups : 2 * groups], refs[2 * groups]
    rows, width = azi[0].shape
    for k in range(groups):
        span = pl.ds(pl.multiple_of((lax.axis_index("mode") ^ k) * width, 128), width)
        out_ref[:rows, span] = rest[k][:rows, :].astype(F32)
        out_ref[rows : 2 * rows, span] = azi[k][...].astype(F32)
        out_ref[2 * rows :, span] = rest[k][rows:, :].astype(F32)


def spread(azi, rest):
    groups = len(azi)
    rows, width = azi[0].shape
    return pl.pallas_call(
        functools.partial(spread_kernel, groups),
        out_shape=jax.ShapeDtypeStruct((3 * rows, groups * width), F32),
        in_specs=[pl.BlockSpec(memory_space=VMEM)] * (2 * groups),
        out_specs=pl.BlockSpec(memory_space=VMEM),
        compiler_params=pltpu.CompilerParams(vmem_limit_bytes=16 * 2**20),
        name="spread",
    )(*azi, *rest)


def fronts_kernel(rows_ref, inv_hbm, cpl_hbm, source_hbm, send_ref, own_ref, source_ref, cpl_v, sems):
    modes, size, _ = cpl_v.shape
    half = modes * size
    copies = [
        pltpu.make_async_copy(inv_hbm, own_ref.at[0], sems.at[0]),
        pltpu.make_async_copy(cpl_hbm, cpl_v, sems.at[1]),
        pltpu.make_async_copy(source_hbm, source_ref, sems.at[2]),
    ]
    for copy in copies:
        copy.start()
    select = one_hot(rows_ref, 1).astype(F32).T.astype(BF16)
    for copy in copies:
        copy.wait()
    for m in range(modes):
        own_ref[1, m] = dot(select, cpl_v[m]).astype(BF16)
        own_ref[2, m] = own_ref[0, m].T
        own_ref[3, m] = own_ref[1, m].T
    send_ref[:half, :] = own_ref[0].reshape(half, size)
    rest = flat(source_ref)
    for part in range(3):
        at = half + part * rest.shape[0]
        term = rest.astype(BF16)
        send_ref[at : at + rest.shape[0], :] = term
        rest = rest - term.astype(F32)


def fronts(rows, inverse, coupling, source):
    modes, size, _ = inverse.shape
    return pl.pallas_call(
        fronts_kernel,
        out_shape=[
            jax.ShapeDtypeStruct((modes * size + 3 * 2 * modes, size), BF16),
            jax.ShapeDtypeStruct((4, modes, size, size), BF16),
            jax.ShapeDtypeStruct(source.shape, F32),
        ],
        in_specs=[pl.BlockSpec(memory_space=VMEM)] + [pl.BlockSpec(memory_space=pltpu.HBM)] * 3,
        out_specs=[pl.BlockSpec(memory_space=VMEM)] * 3,
        scratch_shapes=[VMEM(coupling.shape, BF16), pltpu.SemaphoreType.DMA((3,))],
        compiler_params=pltpu.CompilerParams(vmem_limit_bytes=SMALL),
        name="fronts",
    )(rows, stay(inverse), stay(coupling), stay(source))


def apply(x, matrix):
    modes, size, _ = matrix.shape
    row = lax.broadcasted_iota(jnp.int32, x.shape, 0) % modes
    x = x.astype(F32)
    wide = jnp.concatenate([jnp.where(row == m, x, 0.0).astype(BF16) for m in range(modes)], axis=1)
    return dot(wide, matrix.reshape(modes * size, size))


def apply_turned(x, matrix):
    modes, size, _ = matrix.shape
    wide = dot(x, matrix.reshape(modes * size, size), NT)
    row = lax.broadcasted_iota(jnp.int32, x.shape, 0) % modes
    total = jnp.zeros(x.shape, F32)
    for m in range(modes):
        total += jnp.where(row == m, wide[:, m * size : (m + 1) * size], 0.0)
    return total


def flat(ref):
    return ref[...].reshape(ref.shape[0] * ref.shape[1], ref.shape[2])


def small_call(kernel, outs, args):
    return pl.pallas_call(
        kernel,
        out_shape=outs,
        in_specs=[pl.BlockSpec(memory_space=VMEM)] * len(args),
        out_specs=[pl.BlockSpec(memory_space=VMEM)] * len(outs),
        compiler_params=pltpu.CompilerParams(vmem_limit_bytes=SMALL),
    )(*args)


def rise_kernel(one_ref, two_ref, source_ref, front_ref, reduced_ref, outgoing_ref):
    g = (flat(source_ref) - (flat(one_ref) + flat(two_ref))).astype(BF16)
    reduced = apply(g, front_ref[2]).astype(BF16)
    reduced_ref[...] = reduced.astype(F32).reshape(reduced_ref.shape)
    outgoing_ref[...] = apply(reduced, front_ref[3]).reshape(outgoing_ref.shape)


def crown_kernel(one_ref, two_ref, source_ref, front_ref, lift_ref, x_ref, x16_ref, top_ref):
    _, modes, size, _ = front_ref.shape
    rows = 2 * modes
    half = modes * size
    g = (flat(source_ref) - (flat(one_ref) + flat(two_ref))).astype(BF16)
    mid = apply(g, front_ref[2]).astype(BF16)
    terms = [lift_ref[half + p * rows : half + (p + 1) * rows, :].astype(F32) for p in range(3)]
    g = (terms[0] + terms[1] + terms[2] - apply(mid, front_ref[3])).astype(BF16)
    inverse = lift_ref[:half, :].reshape(modes, size, size)
    top = apply(apply_turned(g, inverse).astype(BF16), inverse)
    top_ref[...] = top.reshape(top_ref.shape)
    residue = mid.astype(F32) - apply(top.astype(BF16), front_ref[1])
    x = apply(residue.astype(BF16), front_ref[0])
    x_ref[...] = x.reshape(x_ref.shape)
    x16_ref[...] = x.astype(BF16).reshape(x_ref.shape)


def sink_kernel(one_ref, two_ref, reduced_ref, front_ref, x_ref, x16_ref):
    above = (flat(one_ref).astype(F32) + flat(two_ref).astype(F32)).astype(BF16)
    residue = flat(reduced_ref) - apply(above, front_ref[1])
    x = apply(residue.astype(BF16), front_ref[0])
    x_ref[...] = x.reshape(x_ref.shape)
    x16_ref[...] = x.astype(BF16).reshape(x_ref.shape)


def level_of(q, levels):
    return levels + 1 if q == 0 else (q & -q).bit_length()


def choose_kernel(*refs):
    position = lax.axis_index("mesh")
    last = len(refs) - 2
    for at, ref in enumerate(refs[:-1]):
        here = position % 2**at == 0
        if at < last:
            here &= position % 2 ** (at + 1) != 0

        @pl.when(here)
        def _(ref=ref):
            refs[-1][...] = ref[...]


def shards(
    velocity,
    magnetic,
    leaf_inverse,
    leaf_coupling,
    separator_inverse,
    separator_coupling,
    separator_source,
    front_rows,
):
    groups = lax.axis_size("mode")
    partitions = lax.axis_size("mesh")
    levels = partitions.bit_length() - 1
    modes, nodes = velocity.shape[2], velocity.shape[3]
    exchange = [[(g, g ^ k) for g in range(groups)] for k in range(groups)]
    mid = partitions // 2

    def swap(pieces):
        out = [pieces[0]]
        for k in range(1, groups):
            out.append(lax.ppermute(pieces[k], "mode", exchange[k]))
        return out

    def hop(value, pairs):
        return lax.ppermute(value, "mesh", pairs)

    *packed, mag = pack(
        stay(velocity.reshape(6 * modes, nodes)), stay(magnetic.reshape(6 * modes, nodes)), groups
    )
    spread_in = swap(packed)
    fwd, bwd = tables(groups, modes)
    send, front, sep_source = fronts(
        front_rows, separator_inverse, separator_coupling, separator_source
    )
    square, joint = compose(stay(leaf_inverse), stay(leaf_coupling))
    azi, rest = transform(fwd, bwd, spread_in)
    azi = swap(azi)
    lift = hop(send, [(0, mid)])
    rest = swap(rest)
    source, update = leaf_up(front_rows, mag, azi, joint)
    local = leaf_local(source, square)
    nonlinear = spread(azi, rest).reshape(3, 2, modes, nodes)

    of_level = [[q for q in range(partitions) if level_of(q, levels) == h] for h in range(levels + 2)]
    wide = jax.ShapeDtypeStruct(separator_source.shape, F32)
    half = jax.ShapeDtypeStruct(separator_source.shape, BF16)
    reduced = [None] * (levels + 1)
    one, two = update, hop(update, [(q - 1, q) for q in of_level[1]])
    for height in range(1, levels):
        reduced[height], outgoing = small_call(
            rise_kernel, [wide, wide], [one, two, sep_source, front]
        )
        gap = 2 ** (height - 1)
        one = hop(outgoing, [(q - gap, q) for q in of_level[height + 1]])
        two = hop(outgoing, [(q + gap, q) for q in of_level[height + 1]])
    x, x16, top = small_call(crown_kernel, [wide, half, wide], [one, two, sep_source, front, lift])
    answers = [(levels, x)]
    for height in range(levels - 1, 0, -1):
        gap = 2 ** (height - 1)
        one = hop(x16, [(q, q - gap) for q in of_level[height + 1]])
        two = hop(x16, [(q, q + gap) for q in of_level[height + 1]])
        x, x16 = small_call(sink_kernel, [wide, half], [one, two, reduced[height], front])
        answers.append((height, x))
    far = hop(top, [(mid, 0)])
    beside = hop(x16, [(q, q - 1) for q in of_level[1]])
    azimuthal = leaf_down(front_rows, x16, beside, local, joint)
    answers.reverse()
    (solution,) = small_call(choose_kernel, [wide], [x for _, x in answers] + [far])
    return (nonlinear, azimuthal, solution)


def solution(mesh):
    in_specs = (
        P(None, None, "mode", "mesh"),
        P(None, None, "mode", "mesh"),
        P("mode", "mesh", None, None),
        P("mode", None, "mesh"),
        P("mode", "mesh", None),
        P("mode", "mesh", None),
        P(None, "mode", "mesh"),
        P("mesh", None, None),
    )
    out_specs = (P(None, None, "mode", "mesh"), P(None, "mode", "mesh"), P(None, "mode", "mesh"))


    return jax.shard_map(shards, mesh=mesh, in_specs=in_specs, out_specs=out_specs, check_vma=False)
```

```python
import functools

import jax
import jax.numpy as jnp
from jax import lax
from jax.experimental import pallas as pl
from jax.experimental.pallas import tpu as pltpu
from jax.sharding import PartitionSpec as P


NPHI = 192
DT_STEP = 0.5
VMEM = pltpu.VMEM
BF16 = jnp.bfloat16
F32 = jnp.float32
NT = (((1,), (1,)), ((), ()))
NN = (((1,), (0,)), ((), ()))
SMALL = 8 * 2**20
LARGE = 8 * 2**20
COMPOSE = 8 * 2**20


def stay(value):
    return pltpu.with_memory_space_constraint(value, pltpu.HBM)


def dot(a, b, dims=NN, precision=None):
    return lax.dot_general(a, b, dims, precision=precision, preferred_element_type=F32)


def tables_kernel(modes, fwd_ref, bwd_ref):
    shape = fwd_ref.shape
    angle = lax.broadcasted_iota(jnp.int32, shape, 0)
    at = lax.broadcasted_iota(jnp.int32, shape, 1)
    step, kind, mode = at // (2 * modes), (at // modes) % 2, at % modes
    order = jnp.bitwise_xor(step, lax.axis_index("mode")) * modes + mode
    turn = (angle * order).astype(F32) + jnp.where(kind == 0, NPHI / 4, 0.0)
    turn = turn - NPHI * jnp.floor((turn + 0.5) * (1.0 / NPHI))
    value = jnp.sin(turn * (2.0 * jnp.pi / NPHI))
    fwd_ref[...] = value.astype(BF16)
    bwd_ref[...] = (value * (jnp.where(order == 0, 1.0, 2.0) / NPHI)).T.astype(BF16)


def tables(groups, modes):
    rows = groups * 2 * modes
    return pl.pallas_call(
        functools.partial(tables_kernel, modes),
        out_shape=[jax.ShapeDtypeStruct((NPHI, rows), BF16), jax.ShapeDtypeStruct((rows, NPHI), BF16)],
        out_specs=[pl.BlockSpec(memory_space=VMEM)] * 2,
        compiler_params=pltpu.CompilerParams(vmem_limit_bytes=SMALL),
        name="tables",
    )()


def pack_kernel(groups, v_hbm, b_hbm, *refs):
    outs, azi_ref, held, sems = refs[:groups], refs[groups], refs[groups + 1], refs[groups + 2]
    rows, width = v_hbm.shape[0], outs[0].shape[1]
    part = rows // 3

    def copy(field, k):
        span = pl.ds(pl.multiple_of((lax.axis_index("mode") ^ k) * width, 128), width)
        source = (v_hbm, b_hbm)[field].at[:, span]
        return pltpu.make_async_copy(source, held.at[k, field], sems.at[k, field])

    order = list(range(1, groups)) + [0]
    for k in order:
        for field in range(2):
            copy(field, k).start()
    for k in order:
        for field in range(2):
            copy(field, k).wait()
            outs[k][field * rows : (field + 1) * rows, :] = held[k, field].astype(BF16)
    for k in order:
        span = pl.ds(pl.multiple_of((lax.axis_index("mode") ^ k) * width, 128), width)
        azi_ref[:, span] = held[k, 1, part : 2 * part]


def pack(velocity, magnetic, groups):
    rows, nodes = velocity.shape
    width = nodes // groups
    return pl.pallas_call(
        functools.partial(pack_kernel, groups),
        out_shape=[jax.ShapeDtypeStruct((2 * rows, width), BF16)] * groups
        + [jax.ShapeDtypeStruct((rows // 3, nodes), F32)],
        in_specs=[pl.BlockSpec(memory_space=pltpu.HBM)] * 2,
        out_specs=[pl.BlockSpec(memory_space=VMEM)] * (groups + 1),
        scratch_shapes=[VMEM((groups, 2, rows, width), F32), pltpu.SemaphoreType.DMA((groups, 2))],
        compiler_params=pltpu.CompilerParams(vmem_limit_bytes=SMALL),
        name="pack",
    )(velocity, magnetic)


def transform_kernel(groups, fwd_ref, bwd_ref, *refs):
    ins, azi, rest = refs[:groups], refs[groups : 2 * groups], refs[2 * groups :]
    rows = ins[0].shape[0] // 6
    fwd, bwd = fwd_ref[...], bwd_ref[...]
    phys = []
    for field in range(6):
        coef = jnp.concatenate([r[field * rows : (field + 1) * rows, :] for r in ins], axis=0)
        phys.append(dot(fwd, coef))
    v, b = phys[:3], phys[3:]
    for c in range(3):
        p, q = (c + 1) % 3, (c + 2) % 3
        crossed = (v[p] * b[q] - v[q] * b[p]).astype(BF16)
        terms = dot(bwd, crossed).astype(BF16)
        for k in range(groups):
            block = terms[k * rows : (k + 1) * rows, :]
            if c == 1:
                azi[k][...] = block
            else:
                at = 0 if c == 0 else rows
                rest[k][at : at + rows, :] = block


def transform(fwd, bwd, pieces):
    groups = len(pieces)
    rows, width = pieces[0].shape
    rows = rows // 6
    out = pl.pallas_call(
        functools.partial(transform_kernel, groups),
        out_shape=[jax.ShapeDtypeStruct((rows, width), BF16)] * groups
        + [jax.ShapeDtypeStruct((2 * rows, width), BF16)] * groups,
        in_specs=[pl.BlockSpec(memory_space=VMEM)] * (2 + groups),
        out_specs=[pl.BlockSpec(memory_space=VMEM)] * (2 * groups),
        compiler_params=pltpu.CompilerParams(vmem_limit_bytes=24 * 2**20),
        name="transform",
    )(fwd, bwd, *pieces)
    return out[:groups], out[groups:]


def one_hot(rows_ref, which):
    n = rows_ref.shape[2]
    return lax.broadcasted_iota(jnp.int32, (n, n), 0) == rows_ref[0, which : which + 1, :]


def side_copies(inv_hbm, cpl_hbm, source_hbm, rows_hbm, own_ref, cpl_v, source_ref, rows_ref, sems):
    return [
        pltpu.make_async_copy(inv_hbm, own_ref.at[0], sems.at[0]),
        pltpu.make_async_copy(cpl_hbm, cpl_v, sems.at[1]),
        pltpu.make_async_copy(source_hbm, source_ref, sems.at[2]),
        pltpu.make_async_copy(rows_hbm, rows_ref, sems.at[3]),
    ]


def prepare_front(rows_ref, send_ref, own_ref, source_ref, cpl_v):
    modes, size, _ = cpl_v.shape
    half = modes * size
    select = one_hot(rows_ref, 1).astype(F32).T.astype(BF16)
    for m in range(modes):
        own_ref[1, m] = dot(select, cpl_v[m]).astype(BF16)
        own_ref[2, m] = own_ref[0, m].T
        own_ref[3, m] = own_ref[1, m].T
    send_ref[:half, :] = own_ref[0].reshape(half, size)
    rest = flat(source_ref)
    for part in range(3):
        at = half + part * rest.shape[0]
        term = rest.astype(BF16)
        send_ref[at : at + rest.shape[0], :] = term
        rest = rest - term.astype(F32)


def compose_kernel(
    rows_hbm, inv_hbm, cpl_hbm, sep_hbm, up_hbm, src_hbm,
    square_ref, joint_ref, send_ref, own_ref, source_ref, rows_ref,
    inv_v, cpl_v, sems, up_v, side_sems,
):
    side = side_copies(sep_hbm, up_hbm, src_hbm, rows_hbm, own_ref, up_v, source_ref, rows_ref, side_sems)
    modes, front, _ = joint_ref.shape
    blocks, size = inv_v.shape[1], inv_v.shape[2]
    depth = inv_v.shape[0]
    zero = jnp.zeros((size, size), BF16)

    def copies(m):
        slot = m % depth
        return (
            pltpu.make_async_copy(inv_hbm.at[m], inv_v.at[slot], sems.at[0, slot]),
            pltpu.make_async_copy(cpl_hbm.at[m], cpl_v.at[slot], sems.at[1, slot]),
        )

    for m in range(depth):
        for copy in copies(m):
            copy.start()

    def one_mode(m, carry):
        slot = m % depth
        for copy in copies(m):
            copy.wait()
        for b in range(0, blocks, 2):
            first, second = inv_v[slot, b], inv_v[slot, b + 1]
            weights = jnp.concatenate(
                [jnp.concatenate([first, zero], axis=1), jnp.concatenate([zero, second], axis=1)],
                axis=0,
            )
            span = slice(b * size, (b + 2) * size)
            rows = jnp.concatenate(
                [cpl_v[slot, :, span], jnp.concatenate([first.T, second.T], axis=1)], axis=0
            )
            out = dot(rows, weights).astype(BF16)
            joint_ref[m, :, span] = out[:front]
            square_ref[m, b] = out[front:, :size]
            square_ref[m, b + 1] = out[front:, size:]

        @pl.when(m + depth < modes)
        def _():
            for copy in copies(m + depth):
                copy.start()

        return carry

    for copy in side:
        copy.start()
    lax.fori_loop(0, modes, one_mode, 0)
    for copy in side:
        copy.wait()
    prepare_front(rows_ref, send_ref, own_ref, source_ref, up_v)


def compose(rows, inverse, coupling, sep_inverse, sep_coupling, source, depth=4):
    count = source.shape[0]
    size_s = source.shape[2]
    modes, blocks, size, _ = inverse.shape
    front, nodes = coupling.shape[1:]
    return pl.pallas_call(
        compose_kernel,
        out_shape=[
            jax.ShapeDtypeStruct(inverse.shape, BF16),
            jax.ShapeDtypeStruct(coupling.shape, BF16),
            jax.ShapeDtypeStruct((modes * size_s + 3 * count * modes, size_s), BF16),
            jax.ShapeDtypeStruct((4, modes, size_s, size_s), BF16),
            jax.ShapeDtypeStruct(source.shape, F32),
            jax.ShapeDtypeStruct(rows.shape, rows.dtype),
        ],
        in_specs=[pl.BlockSpec(memory_space=pltpu.HBM)] * 6,
        out_specs=[pl.BlockSpec(memory_space=VMEM)] * 6,
        scratch_shapes=[
            VMEM((depth, blocks, size, size), BF16),
            VMEM((depth, front, nodes), BF16),
            pltpu.SemaphoreType.DMA((2, depth)),
            VMEM(sep_coupling.shape, BF16),
            pltpu.SemaphoreType.DMA((4,)),
        ],
        compiler_params=pltpu.CompilerParams(vmem_limit_bytes=COMPOSE),
        cost_estimate=pl.CostEstimate(
            flops=4 * modes * nodes * size * (front + size),
            bytes_accessed=4 * (inverse.size + coupling.size),
            transcendentals=0,
        ),
        name="compose",
    )(*(stay(value) for value in (rows, inverse, coupling, sep_inverse, sep_coupling, source)))


def leaf_up_kernel(groups, rows_ref, mag_ref, joint_ref, *refs):
    pieces = refs[:groups]
    source_ref, update_ref, turned_v = refs[groups:]
    modes, front, nodes = joint_ref.shape
    width = nodes // groups
    for k in range(groups):
        at = pl.multiple_of((lax.axis_index("mode") ^ k) * width, 128)
        span = pl.ds(at, width)
        source = (mag_ref[:, span] + DT_STEP * pieces[k][...].astype(F32)).astype(BF16)
        source_ref[:, :, span] = source.astype(F32).reshape(2, modes, width)
        turned_v[pl.ds(at, width), :] = source.T
    turned = turned_v[...]
    lane = lax.broadcasted_iota(jnp.int32, (front, 2 * modes), 1) % modes

    def one_mode(m, total):
        return total + jnp.where(lane == m, dot(joint_ref[m], turned), 0.0)

    total = lax.fori_loop(0, modes, one_mode, jnp.zeros((front, 2 * modes), F32), unroll=4)
    select = one_hot(rows_ref, 0).astype(F32)
    update_ref[...] = dot(total.T, select, precision=lax.Precision.HIGHEST).reshape(update_ref.shape)


def leaf_up(rows, mag, pieces, joint):
    modes, front, nodes = joint.shape
    groups = len(pieces)
    whole = pl.BlockSpec(memory_space=VMEM)
    return pl.pallas_call(
        functools.partial(leaf_up_kernel, groups),
        out_shape=[
            jax.ShapeDtypeStruct((2, modes, nodes), F32),
            jax.ShapeDtypeStruct((2, modes, front), F32),
        ],
        in_specs=[whole] * (3 + groups),
        out_specs=[whole] * 2,
        scratch_shapes=[VMEM((nodes, 2 * modes), BF16)],
        compiler_params=pltpu.CompilerParams(vmem_limit_bytes=LARGE),
        cost_estimate=pl.CostEstimate(
            flops=128 * modes * nodes * front, bytes_accessed=2 * joint.size, transcendentals=0
        ),
        name="leaf_up",
    )(rows, mag, joint, *pieces)


def leaf_local_kernel(source_ref, square_ref, out_ref):
    modes, blocks, size, _ = square_ref.shape
    nodes = blocks * size
    zero = jnp.zeros((2, size), BF16)

    def one_mode(m, carry):
        source = source_ref[:, pl.ds(m, 1), :].reshape(2, nodes).astype(BF16)
        parts = []
        for b in range(0, blocks, 2):
            one = source[:, b * size : (b + 1) * size]
            two = source[:, (b + 1) * size : (b + 2) * size]
            left = jnp.concatenate(
                [jnp.concatenate([one, zero], axis=1), jnp.concatenate([zero, two], axis=1)], axis=0
            )
            pair = dot(left, square_ref[m, b : b + 2].reshape(2 * size, size))
            parts += [pair[:2], pair[2:]]
        out_ref[:, pl.ds(m, 1), :] = jnp.concatenate(parts, axis=1).reshape(2, 1, nodes)
        return carry

    lax.fori_loop(0, modes, one_mode, 0, unroll=2)


def leaf_local(source, square):
    whole = pl.BlockSpec(memory_space=VMEM)
    return pl.pallas_call(
        leaf_local_kernel,
        out_shape=jax.ShapeDtypeStruct(source.shape, F32),
        in_specs=[whole] * 2,
        out_specs=whole,
        compiler_params=pltpu.CompilerParams(vmem_limit_bytes=LARGE),
        cost_estimate=pl.CostEstimate(
            flops=128 * square.size, bytes_accessed=2 * square.size, transcendentals=0
        ),
        name="leaf_local",
    )(source, square)


def leaf_down_kernel(rows_ref, here_ref, beside_ref, local_ref, joint_ref, out_ref, x_v):
    modes, front, nodes = joint_ref.shape
    select = one_hot(rows_ref, 0).astype(F32).astype(BF16)
    above = jnp.where(lax.axis_index("mesh") % 2 == 1, here_ref[...].astype(F32), beside_ref[...].astype(F32))
    x_v[...] = dot(above.reshape(2 * modes, front).astype(BF16), select, NT).reshape(2, modes, front)
    zero = jnp.zeros((2, front), F32)

    def two_modes(i, carry):
        one = x_v[:, pl.ds(2 * i, 1), :].reshape(2, front)
        two = x_v[:, pl.ds(2 * i + 1, 1), :].reshape(2, front)
        left = jnp.concatenate(
            [jnp.concatenate([one, zero], axis=1), jnp.concatenate([zero, two], axis=1)], axis=0
        ).astype(BF16)
        out = dot(left, joint_ref[pl.ds(2 * i, 2)].reshape(2 * front, nodes))
        for half in range(2):
            place = pl.ds(2 * i + half, 1)
            value = local_ref[:, place, :].reshape(2, nodes) - out[2 * half : 2 * half + 2]
            out_ref[:, place, :] = value.reshape(2, 1, nodes)
        return carry

    lax.fori_loop(0, modes // 2, two_modes, 0, unroll=2)


def leaf_down(rows, here, beside, local, joint):
    whole = pl.BlockSpec(memory_space=VMEM)
    return pl.pallas_call(
        leaf_down_kernel,
        out_shape=jax.ShapeDtypeStruct(local.shape, F32),
        in_specs=[whole] * 5,
        out_specs=whole,
        scratch_shapes=[VMEM(here.shape, F32)],
        compiler_params=pltpu.CompilerParams(vmem_limit_bytes=LARGE),
        name="leaf_down",
    )(rows, here, beside, local, joint)


def spread_kernel(groups, *refs):
    azi, rest, out_ref = refs[:groups], refs[groups : 2 * groups], refs[2 * groups]
    rows, width = azi[0].shape
    for k in range(groups):
        span = pl.ds(pl.multiple_of((lax.axis_index("mode") ^ k) * width, 128), width)
        out_ref[:rows, span] = rest[k][:rows, :].astype(F32)
        out_ref[rows : 2 * rows, span] = azi[k][...].astype(F32)
        out_ref[2 * rows :, span] = rest[k][rows:, :].astype(F32)


def spread(azi, rest):
    groups = len(azi)
    rows, width = azi[0].shape
    return pl.pallas_call(
        functools.partial(spread_kernel, groups),
        out_shape=jax.ShapeDtypeStruct((3 * rows, groups * width), F32),
        in_specs=[pl.BlockSpec(memory_space=VMEM)] * (2 * groups),
        out_specs=pl.BlockSpec(memory_space=VMEM),
        compiler_params=pltpu.CompilerParams(vmem_limit_bytes=16 * 2**20),
        name="spread",
    )(*azi, *rest)


def apply(x, matrix):
    modes, size, _ = matrix.shape
    row = lax.broadcasted_iota(jnp.int32, x.shape, 0) % modes
    x = x.astype(F32)
    wide = jnp.concatenate([jnp.where(row == m, x, 0.0).astype(BF16) for m in range(modes)], axis=1)
    return dot(wide, matrix.reshape(modes * size, size))


def apply_turned(x, matrix):
    modes, size, _ = matrix.shape
    wide = dot(x, matrix.reshape(modes * size, size), NT)
    row = lax.broadcasted_iota(jnp.int32, x.shape, 0) % modes
    total = jnp.zeros(x.shape, F32)
    for m in range(modes):
        total += jnp.where(row == m, wide[:, m * size : (m + 1) * size], 0.0)
    return total


def flat(ref):
    return ref[...].reshape(ref.shape[0] * ref.shape[1], ref.shape[2])


def small_call(kernel, outs, args):
    return pl.pallas_call(
        kernel,
        out_shape=outs,
        in_specs=[pl.BlockSpec(memory_space=VMEM)] * len(args),
        out_specs=[pl.BlockSpec(memory_space=VMEM)] * len(outs),
        compiler_params=pltpu.CompilerParams(vmem_limit_bytes=SMALL),
    )(*args)


def rise_kernel(one_ref, two_ref, source_ref, front_ref, reduced_ref, outgoing_ref):
    g = (flat(source_ref) - (flat(one_ref) + flat(two_ref))).astype(BF16)
    reduced = apply(g, front_ref[2]).astype(BF16)
    reduced_ref[...] = reduced.astype(F32).reshape(reduced_ref.shape)
    outgoing_ref[...] = apply(reduced, front_ref[3]).reshape(outgoing_ref.shape)


def crown_kernel(one_ref, two_ref, source_ref, front_ref, lift_ref, x_ref, x16_ref, top_ref):
    _, modes, size, _ = front_ref.shape
    rows = 2 * modes
    half = modes * size
    g = (flat(source_ref) - (flat(one_ref) + flat(two_ref))).astype(BF16)
    mid = apply(g, front_ref[2]).astype(BF16)
    terms = [lift_ref[half + p * rows : half + (p + 1) * rows, :].astype(F32) for p in range(3)]
    g = (terms[0] + terms[1] + terms[2] - apply(mid, front_ref[3])).astype(BF16)
    inverse = lift_ref[:half, :].reshape(modes, size, size)
    top = apply(apply_turned(g, inverse).astype(BF16), inverse)
    top_ref[...] = top.reshape(top_ref.shape)
    residue = mid.astype(F32) - apply(top.astype(BF16), front_ref[1])
    x = apply(residue.astype(BF16), front_ref[0])
    x_ref[...] = x.reshape(x_ref.shape)
    x16_ref[...] = x.astype(BF16).reshape(x_ref.shape)


def sink_kernel(one_ref, two_ref, reduced_ref, front_ref, x_ref, x16_ref):
    above = (flat(one_ref).astype(F32) + flat(two_ref).astype(F32)).astype(BF16)
    residue = flat(reduced_ref) - apply(above, front_ref[1])
    x = apply(residue.astype(BF16), front_ref[0])
    x_ref[...] = x.reshape(x_ref.shape)
    x16_ref[...] = x.astype(BF16).reshape(x_ref.shape)


def level_of(q, levels):
    return levels + 1 if q == 0 else (q & -q).bit_length()


def choose_kernel(*refs):
    position = lax.axis_index("mesh")
    last = len(refs) - 2
    for at, ref in enumerate(refs[:-1]):
        here = position % 2**at == 0
        if at < last:
            here &= position % 2 ** (at + 1) != 0

        @pl.when(here)
        def _(ref=ref):
            refs[-1][...] = ref[...]


def shards(
    velocity,
    magnetic,
    leaf_inverse,
    leaf_coupling,
    separator_inverse,
    separator_coupling,
    separator_source,
    front_rows,
):
    groups = lax.axis_size("mode")
    partitions = lax.axis_size("mesh")
    levels = partitions.bit_length() - 1
    modes, nodes = velocity.shape[2], velocity.shape[3]
    exchange = [[(g, g ^ k) for g in range(groups)] for k in range(groups)]
    mid = partitions // 2

    def swap(pieces):
        out = [pieces[0]]
        for k in range(1, groups):
            out.append(lax.ppermute(pieces[k], "mode", exchange[k]))
        return out

    def hop(value, pairs):
        return lax.ppermute(value, "mesh", pairs)

    *packed, mag = pack(
        stay(velocity.reshape(6 * modes, nodes)), stay(magnetic.reshape(6 * modes, nodes)), groups
    )
    spread_in = swap(packed)
    fwd, bwd = tables(groups, modes)
    square, joint, send, front, sep_source, rows = compose(
        front_rows, leaf_inverse, leaf_coupling, separator_inverse, separator_coupling, separator_source
    )
    azi, rest = transform(fwd, bwd, spread_in)
    azi = swap(azi)
    lift = hop(send, [(0, mid)])
    rest = swap(rest)
    source, update = leaf_up(rows, mag, azi, joint)
    local = leaf_local(source, square)
    nonlinear = spread(azi, rest).reshape(3, 2, modes, nodes)

    of_level = [[q for q in range(partitions) if level_of(q, levels) == h] for h in range(levels + 2)]
    wide = jax.ShapeDtypeStruct(separator_source.shape, F32)
    half = jax.ShapeDtypeStruct(separator_source.shape, BF16)
    reduced = [None] * (levels + 1)
    one, two = update, hop(update, [(q - 1, q) for q in of_level[1]])
    for height in range(1, levels):
        reduced[height], outgoing = small_call(rise_kernel, [wide, wide], [one, two, sep_source, front])
        gap = 2 ** (height - 1)
        one = hop(outgoing, [(q - gap, q) for q in of_level[height + 1]])
        two = hop(outgoing, [(q + gap, q) for q in of_level[height + 1]])
    x, x16, top = small_call(crown_kernel, [wide, half, wide], [one, two, sep_source, front, lift])
    answers = [(levels, x)]
    for height in range(levels - 1, 0, -1):
        gap = 2 ** (height - 1)
        one = hop(x16, [(q, q - gap) for q in of_level[height + 1]])
        two = hop(x16, [(q, q + gap) for q in of_level[height + 1]])
        x, x16 = small_call(sink_kernel, [wide, half], [one, two, reduced[height], front])
        answers.append((height, x))
    far = hop(top, [(mid, 0)])
    beside = hop(x16, [(q, q - 1) for q in of_level[1]])
    azimuthal = leaf_down(rows, x16, beside, local, joint)
    answers.reverse()
    (solution,) = small_call(choose_kernel, [wide], [x for _, x in answers] + [far])
    return (nonlinear, azimuthal, solution)


def solution(mesh):
    in_specs = (
        P(None, None, "mode", "mesh"),
        P(None, None, "mode", "mesh"),
        P("mode", "mesh", None, None),
        P("mode", None, "mesh"),
        P("mode", "mesh", None),
        P("mode", "mesh", None),
        P(None, "mode", "mesh"),
        P("mesh", None, None),
    )
    out_specs = (P(None, None, "mode", "mesh"), P(None, "mode", "mesh"), P(None, "mode", "mesh"))


    return jax.shard_map(shards, mesh=mesh, in_specs=in_specs, out_specs=out_specs, check_vma=False)
```

```python
import functools

import jax
import jax.numpy as jnp
from jax import lax
from jax.experimental import pallas as pl
from jax.experimental.pallas import tpu as pltpu
from jax.sharding import PartitionSpec as P


NPHI = 192
DT_STEP = 0.5
VMEM = pltpu.VMEM
BF16 = jnp.bfloat16
F32 = jnp.float32
NT = (((1,), (1,)), ((), ()))
NN = (((1,), (0,)), ((), ()))
SMALL = 8 * 2**20
LARGE = 8 * 2**20
COMPOSE = 8 * 2**20


def stay(value):
    return pltpu.with_memory_space_constraint(value, pltpu.HBM)


def dot(a, b, dims=NN, precision=None):
    return lax.dot_general(a, b, dims, precision=precision, preferred_element_type=F32)


def tables_kernel(modes, fwd_ref, bwd_ref):
    shape = fwd_ref.shape
    angle = lax.broadcasted_iota(jnp.int32, shape, 0)
    at = lax.broadcasted_iota(jnp.int32, shape, 1)
    step, kind, mode = at // (2 * modes), (at // modes) % 2, at % modes
    order = jnp.bitwise_xor(step, lax.axis_index("mode")) * modes + mode
    turn = (angle * order).astype(F32) + jnp.where(kind == 0, NPHI / 4, 0.0)
    turn = turn - NPHI * jnp.floor((turn + 0.5) * (1.0 / NPHI))
    value = jnp.sin(turn * (2.0 * jnp.pi / NPHI))
    fwd_ref[...] = value.astype(BF16)
    bwd_ref[...] = (value * (jnp.where(order == 0, 1.0, 2.0) / NPHI)).T.astype(BF16)


def tables(groups, modes):
    rows = groups * 2 * modes
    return pl.pallas_call(
        functools.partial(tables_kernel, modes),
        out_shape=[jax.ShapeDtypeStruct((NPHI, rows), BF16), jax.ShapeDtypeStruct((rows, NPHI), BF16)],
        out_specs=[pl.BlockSpec(memory_space=VMEM)] * 2,
        compiler_params=pltpu.CompilerParams(vmem_limit_bytes=SMALL),
        name="tables",
    )()


def pack_kernel(groups, v_hbm, b_hbm, *refs):
    outs, azi_ref, held, sems = refs[:groups], refs[groups], refs[groups + 1], refs[groups + 2]
    rows, width = v_hbm.shape[0], outs[0].shape[1]
    part = rows // 3

    def copy(field, k):
        span = pl.ds(pl.multiple_of((lax.axis_index("mode") ^ k) * width, 128), width)
        source = (v_hbm, b_hbm)[field].at[:, span]
        return pltpu.make_async_copy(source, held.at[k, field], sems.at[k, field])

    order = list(range(1, groups)) + [0]
    for k in order:
        for field in range(2):
            copy(field, k).start()
    for k in order:
        for field in range(2):
            copy(field, k).wait()
            outs[k][field * rows : (field + 1) * rows, :] = held[k, field].astype(BF16)
    for k in order:
        span = pl.ds(pl.multiple_of((lax.axis_index("mode") ^ k) * width, 128), width)
        azi_ref[:, span] = held[k, 1, part : 2 * part]


def pack(velocity, magnetic, groups):
    rows, nodes = velocity.shape
    width = nodes // groups
    return pl.pallas_call(
        functools.partial(pack_kernel, groups),
        out_shape=[jax.ShapeDtypeStruct((2 * rows, width), BF16)] * groups
        + [jax.ShapeDtypeStruct((rows // 3, nodes), F32)],
        in_specs=[pl.BlockSpec(memory_space=pltpu.HBM)] * 2,
        out_specs=[pl.BlockSpec(memory_space=VMEM)] * (groups + 1),
        scratch_shapes=[VMEM((groups, 2, rows, width), F32), pltpu.SemaphoreType.DMA((groups, 2))],
        compiler_params=pltpu.CompilerParams(vmem_limit_bytes=SMALL),
        name="pack",
    )(velocity, magnetic)


def transform_kernel(groups, components, fwd_ref, bwd_ref, *refs):
    ins, outs = refs[:groups], refs[groups:]
    rows = ins[0].shape[0] // 6
    fwd, bwd = fwd_ref[...], bwd_ref[...]
    used = sorted({(c + s) % 3 for c in components for s in (1, 2)})

    def phys(field):
        coef = jnp.concatenate([r[field * rows : (field + 1) * rows, :] for r in ins], axis=0)
        return dot(fwd, coef)

    v, b = {c: phys(c) for c in used}, {c: phys(3 + c) for c in used}
    for at, c in enumerate(components):
        p, q = (c + 1) % 3, (c + 2) % 3
        crossed = (v[p] * b[q] - v[q] * b[p]).astype(BF16)
        terms = dot(bwd, crossed).astype(BF16)
        for k in range(groups):
            outs[k][at * rows : (at + 1) * rows, :] = terms[k * rows : (k + 1) * rows, :]


def transform(fwd, bwd, pieces, components):
    groups = len(pieces)
    rows, width = pieces[0].shape
    rows = rows // 6 * len(components)
    return pl.pallas_call(
        functools.partial(transform_kernel, groups, components),
        out_shape=[jax.ShapeDtypeStruct((rows, width), BF16)] * groups,
        in_specs=[pl.BlockSpec(memory_space=VMEM)] * (2 + groups),
        out_specs=[pl.BlockSpec(memory_space=VMEM)] * groups,
        compiler_params=pltpu.CompilerParams(vmem_limit_bytes=24 * 2**20),
        name="transform",
    )(fwd, bwd, *pieces)


def one_hot(rows_ref, which):
    n = rows_ref.shape[2]
    return lax.broadcasted_iota(jnp.int32, (n, n), 0) == rows_ref[0, which : which + 1, :]


def side_copies(inv_hbm, cpl_hbm, source_hbm, rows_hbm, own_ref, cpl_v, source_ref, rows_ref, sems):
    return [
        pltpu.make_async_copy(inv_hbm, own_ref.at[0], sems.at[0]),
        pltpu.make_async_copy(cpl_hbm, cpl_v, sems.at[1]),
        pltpu.make_async_copy(source_hbm, source_ref, sems.at[2]),
        pltpu.make_async_copy(rows_hbm, rows_ref, sems.at[3]),
    ]


def prepare_front(rows_ref, send_ref, own_ref, source_ref, cpl_v):
    modes, size, _ = cpl_v.shape
    half = modes * size
    select = one_hot(rows_ref, 1).astype(F32).T.astype(BF16)
    for m in range(modes):
        own_ref[1, m] = dot(select, cpl_v[m]).astype(BF16)
        own_ref[2, m] = own_ref[0, m].T
        own_ref[3, m] = own_ref[1, m].T
    send_ref[:half, :] = own_ref[0].reshape(half, size)
    rest = flat(source_ref)
    for part in range(3):
        at = half + part * rest.shape[0]
        term = rest.astype(BF16)
        send_ref[at : at + rest.shape[0], :] = term
        rest = rest - term.astype(F32)


def compose_kernel(
    rows_hbm, inv_hbm, cpl_hbm, sep_hbm, up_hbm, src_hbm,
    square_ref, joint_ref, send_ref, own_ref, source_ref, rows_ref,
    inv_v, cpl_v, sems, up_v, side_sems,
):
    side = side_copies(sep_hbm, up_hbm, src_hbm, rows_hbm, own_ref, up_v, source_ref, rows_ref, side_sems)
    modes, front, _ = joint_ref.shape
    blocks, size = inv_v.shape[1], inv_v.shape[2]
    depth = inv_v.shape[0]
    zero = jnp.zeros((size, size), BF16)

    def copies(m):
        slot = m % depth
        return (
            pltpu.make_async_copy(inv_hbm.at[m], inv_v.at[slot], sems.at[0, slot]),
            pltpu.make_async_copy(cpl_hbm.at[m], cpl_v.at[slot], sems.at[1, slot]),
        )

    for m in range(depth):
        for copy in copies(m):
            copy.start()

    def one_mode(m, carry):
        slot = m % depth
        for copy in copies(m):
            copy.wait()
        for b in range(0, blocks, 2):
            first, second = inv_v[slot, b], inv_v[slot, b + 1]
            weights = jnp.concatenate(
                [jnp.concatenate([first, zero], axis=1), jnp.concatenate([zero, second], axis=1)],
                axis=0,
            )
            span = slice(b * size, (b + 2) * size)
            rows = jnp.concatenate(
                [cpl_v[slot, :, span], jnp.concatenate([first.T, second.T], axis=1)], axis=0
            )
            out = dot(rows, weights).astype(BF16)
            joint_ref[m, :, span] = out[:front]
            square_ref[m, b] = out[front:, :size]
            square_ref[m, b + 1] = out[front:, size:]

        @pl.when(m + depth < modes)
        def _():
            for copy in copies(m + depth):
                copy.start()

        return carry

    for copy in side:
        copy.start()
    lax.fori_loop(0, modes, one_mode, 0)
    for copy in side:
        copy.wait()
    prepare_front(rows_ref, send_ref, own_ref, source_ref, up_v)


def compose(rows, inverse, coupling, sep_inverse, sep_coupling, source, depth=4):
    count = source.shape[0]
    size_s = source.shape[2]
    modes, blocks, size, _ = inverse.shape
    front, nodes = coupling.shape[1:]
    return pl.pallas_call(
        compose_kernel,
        out_shape=[
            jax.ShapeDtypeStruct(inverse.shape, BF16),
            jax.ShapeDtypeStruct(coupling.shape, BF16),
            jax.ShapeDtypeStruct((modes * size_s + 3 * count * modes, size_s), BF16),
            jax.ShapeDtypeStruct((4, modes, size_s, size_s), BF16),
            jax.ShapeDtypeStruct(source.shape, F32),
            jax.ShapeDtypeStruct(rows.shape, rows.dtype),
        ],
        in_specs=[pl.BlockSpec(memory_space=pltpu.HBM)] * 6,
        out_specs=[pl.BlockSpec(memory_space=VMEM)] * 6,
        scratch_shapes=[
            VMEM((depth, blocks, size, size), BF16),
            VMEM((depth, front, nodes), BF16),
            pltpu.SemaphoreType.DMA((2, depth)),
            VMEM(sep_coupling.shape, BF16),
            pltpu.SemaphoreType.DMA((4,)),
        ],
        compiler_params=pltpu.CompilerParams(vmem_limit_bytes=COMPOSE),
        cost_estimate=pl.CostEstimate(
            flops=4 * modes * nodes * size * (front + size),
            bytes_accessed=4 * (inverse.size + coupling.size),
            transcendentals=0,
        ),
        name="compose",
    )(*(stay(value) for value in (rows, inverse, coupling, sep_inverse, sep_coupling, source)))


def leaf_up_kernel(groups, rows_ref, mag_ref, joint_ref, *refs):
    pieces = refs[:groups]
    source_ref, update_ref, turned_v = refs[groups:]
    modes, front, nodes = joint_ref.shape
    width = nodes // groups
    for k in range(groups):
        at = pl.multiple_of((lax.axis_index("mode") ^ k) * width, 128)
        span = pl.ds(at, width)
        source = (mag_ref[:, span] + DT_STEP * pieces[k][...].astype(F32)).astype(BF16)
        source_ref[:, :, span] = source.astype(F32).reshape(2, modes, width)
        turned_v[pl.ds(at, width), :] = source.T
    turned = turned_v[...]
    lane = lax.broadcasted_iota(jnp.int32, (front, 2 * modes), 1) % modes

    def one_mode(m, total):
        return total + jnp.where(lane == m, dot(joint_ref[m], turned), 0.0)

    total = lax.fori_loop(0, modes, one_mode, jnp.zeros((front, 2 * modes), F32), unroll=4)
    select = one_hot(rows_ref, 0).astype(F32)
    update_ref[...] = dot(total.T, select, precision=lax.Precision.HIGHEST).reshape(update_ref.shape)


def leaf_up(rows, mag, pieces, joint):
    modes, front, nodes = joint.shape
    groups = len(pieces)
    whole = pl.BlockSpec(memory_space=VMEM)
    return pl.pallas_call(
        functools.partial(leaf_up_kernel, groups),
        out_shape=[
            jax.ShapeDtypeStruct((2, modes, nodes), F32),
            jax.ShapeDtypeStruct((2, modes, front), F32),
        ],
        in_specs=[whole] * (3 + groups),
        out_specs=[whole] * 2,
        scratch_shapes=[VMEM((nodes, 2 * modes), BF16)],
        compiler_params=pltpu.CompilerParams(vmem_limit_bytes=LARGE),
        cost_estimate=pl.CostEstimate(
            flops=128 * modes * nodes * front, bytes_accessed=2 * joint.size, transcendentals=0
        ),
        name="leaf_up",
    )(rows, mag, joint, *pieces)


def leaf_local_kernel(source_ref, square_ref, out_ref):
    modes, blocks, size, _ = square_ref.shape
    nodes = blocks * size
    zero = jnp.zeros((2, size), BF16)

    def one_mode(m, carry):
        source = source_ref[:, pl.ds(m, 1), :].reshape(2, nodes).astype(BF16)
        parts = []
        for b in range(0, blocks, 2):
            one = source[:, b * size : (b + 1) * size]
            two = source[:, (b + 1) * size : (b + 2) * size]
            left = jnp.concatenate(
                [jnp.concatenate([one, zero], axis=1), jnp.concatenate([zero, two], axis=1)], axis=0
            )
            pair = dot(left, square_ref[m, b : b + 2].reshape(2 * size, size))
            parts += [pair[:2], pair[2:]]
        out_ref[:, pl.ds(m, 1), :] = jnp.concatenate(parts, axis=1).reshape(2, 1, nodes)
        return carry

    lax.fori_loop(0, modes, one_mode, 0, unroll=2)


def leaf_local(source, square):
    whole = pl.BlockSpec(memory_space=VMEM)
    return pl.pallas_call(
        leaf_local_kernel,
        out_shape=jax.ShapeDtypeStruct(source.shape, F32),
        in_specs=[whole] * 2,
        out_specs=whole,
        compiler_params=pltpu.CompilerParams(vmem_limit_bytes=LARGE),
        cost_estimate=pl.CostEstimate(
            flops=128 * square.size, bytes_accessed=2 * square.size, transcendentals=0
        ),
        name="leaf_local",
    )(source, square)


def leaf_down_kernel(rows_ref, here_ref, beside_ref, local_ref, joint_ref, *refs):
    answers, (out_ref, solution_ref, x_v) = refs[:-3], refs[-3:]
    position = lax.axis_index("mesh")
    for at, ref in enumerate(answers):
        owner = position % 2**at == 0
        if at < len(answers) - 1:
            owner &= position % 2 ** (at + 1) != 0

        @pl.when(owner)
        def _(ref=ref):
            solution_ref[...] = ref[...]

    modes, front, nodes = joint_ref.shape
    select = one_hot(rows_ref, 0).astype(F32).astype(BF16)
    above = jnp.where(lax.axis_index("mesh") % 2 == 1, here_ref[...].astype(F32), beside_ref[...].astype(F32))
    x_v[...] = dot(above.reshape(2 * modes, front).astype(BF16), select, NT).reshape(2, modes, front)
    zero = jnp.zeros((2, front), F32)

    def two_modes(i, carry):
        one = x_v[:, pl.ds(2 * i, 1), :].reshape(2, front)
        two = x_v[:, pl.ds(2 * i + 1, 1), :].reshape(2, front)
        left = jnp.concatenate(
            [jnp.concatenate([one, zero], axis=1), jnp.concatenate([zero, two], axis=1)], axis=0
        ).astype(BF16)
        out = dot(left, joint_ref[pl.ds(2 * i, 2)].reshape(2 * front, nodes))
        for half in range(2):
            place = pl.ds(2 * i + half, 1)
            value = local_ref[:, place, :].reshape(2, nodes) - out[2 * half : 2 * half + 2]
            out_ref[:, place, :] = value.reshape(2, 1, nodes)
        return carry

    lax.fori_loop(0, modes // 2, two_modes, 0, unroll=2)


def leaf_down(rows, here, beside, local, joint, answers):
    whole = pl.BlockSpec(memory_space=VMEM)
    return pl.pallas_call(
        leaf_down_kernel,
        out_shape=[
            jax.ShapeDtypeStruct(local.shape, F32),
            jax.ShapeDtypeStruct(here.shape, F32),
        ],
        in_specs=[whole] * (5 + len(answers)),
        out_specs=[whole] * 2,
        scratch_shapes=[VMEM(here.shape, F32)],
        compiler_params=pltpu.CompilerParams(vmem_limit_bytes=LARGE),
        name="leaf_down",
    )(rows, here, beside, local, joint, *answers)


def spread_kernel(groups, *refs):
    azi, rest, out_ref = refs[:groups], refs[groups : 2 * groups], refs[2 * groups]
    rows, width = azi[0].shape
    for k in range(groups):
        span = pl.ds(pl.multiple_of((lax.axis_index("mode") ^ k) * width, 128), width)
        out_ref[:rows, span] = rest[k][:rows, :].astype(F32)
        out_ref[rows : 2 * rows, span] = azi[k][...].astype(F32)
        out_ref[2 * rows :, span] = rest[k][rows:, :].astype(F32)


def spread(azi, rest):
    groups = len(azi)
    rows, width = azi[0].shape
    return pl.pallas_call(
        functools.partial(spread_kernel, groups),
        out_shape=jax.ShapeDtypeStruct((3 * rows, groups * width), F32),
        in_specs=[pl.BlockSpec(memory_space=VMEM)] * (2 * groups),
        out_specs=pl.BlockSpec(memory_space=VMEM),
        compiler_params=pltpu.CompilerParams(vmem_limit_bytes=16 * 2**20),
        name="spread",
    )(*azi, *rest)


def apply(x, matrix):
    modes, size, _ = matrix.shape
    row = lax.broadcasted_iota(jnp.int32, x.shape, 0) % modes
    x = x.astype(F32)
    wide = jnp.concatenate([jnp.where(row == m, x, 0.0).astype(BF16) for m in range(modes)], axis=1)
    return dot(wide, matrix.reshape(modes * size, size))


def apply_turned(x, matrix):
    modes, size, _ = matrix.shape
    wide = dot(x, matrix.reshape(modes * size, size), NT)
    row = lax.broadcasted_iota(jnp.int32, x.shape, 0) % modes
    total = jnp.zeros(x.shape, F32)
    for m in range(modes):
        total += jnp.where(row == m, wide[:, m * size : (m + 1) * size], 0.0)
    return total


def flat(ref):
    return ref[...].reshape(ref.shape[0] * ref.shape[1], ref.shape[2])


def small_call(kernel, outs, args):
    return pl.pallas_call(
        kernel,
        out_shape=outs,
        in_specs=[pl.BlockSpec(memory_space=VMEM)] * len(args),
        out_specs=[pl.BlockSpec(memory_space=VMEM)] * len(outs),
        compiler_params=pltpu.CompilerParams(vmem_limit_bytes=SMALL),
    )(*args)


def rise_kernel(one_ref, two_ref, source_ref, front_ref, reduced_ref, outgoing_ref):
    g = (flat(source_ref) - (flat(one_ref) + flat(two_ref))).astype(BF16)
    reduced = apply(g, front_ref[2]).astype(BF16)
    reduced_ref[...] = reduced.astype(F32).reshape(reduced_ref.shape)
    outgoing_ref[...] = apply(reduced, front_ref[3]).reshape(outgoing_ref.shape)


def crown_kernel(mid_at, one_ref, two_ref, source_ref, front_ref, lift_ref, x_ref, x16_ref, top_ref):
    @pl.when(lax.axis_index("mesh") == mid_at)
    def _():
        _, modes, size, _ = front_ref.shape
        rows = 2 * modes
        half = modes * size
        g = (flat(source_ref) - (flat(one_ref) + flat(two_ref))).astype(BF16)
        mid = apply(g, front_ref[2]).astype(BF16)
        terms = [lift_ref[half + p * rows : half + (p + 1) * rows, :].astype(F32) for p in range(3)]
        g = (terms[0] + terms[1] + terms[2] - apply(mid, front_ref[3])).astype(BF16)
        inverse = lift_ref[:half, :].reshape(modes, size, size)
        top = apply(apply_turned(g, inverse).astype(BF16), inverse)
        top_ref[...] = top.reshape(top_ref.shape)
        residue = mid.astype(F32) - apply(top.astype(BF16), front_ref[1])
        x = apply(residue.astype(BF16), front_ref[0])
        x_ref[...] = x.reshape(x_ref.shape)
        x16_ref[...] = x.astype(BF16).reshape(x_ref.shape)


def sink_kernel(one_ref, two_ref, reduced_ref, front_ref, x_ref, x16_ref):
    above = (flat(one_ref).astype(F32) + flat(two_ref).astype(F32)).astype(BF16)
    residue = flat(reduced_ref) - apply(above, front_ref[1])
    x = apply(residue.astype(BF16), front_ref[0])
    x_ref[...] = x.reshape(x_ref.shape)
    x16_ref[...] = x.astype(BF16).reshape(x_ref.shape)


def level_of(q, levels):
    return levels + 1 if q == 0 else (q & -q).bit_length()


def shards(
    velocity,
    magnetic,
    leaf_inverse,
    leaf_coupling,
    separator_inverse,
    separator_coupling,
    separator_source,
    front_rows,
):
    groups = lax.axis_size("mode")
    partitions = lax.axis_size("mesh")
    levels = partitions.bit_length() - 1
    modes, nodes = velocity.shape[2], velocity.shape[3]
    exchange = [[(g, g ^ k) for g in range(groups)] for k in range(groups)]
    mid = partitions // 2

    def swap(pieces):
        out = [pieces[0]]
        for k in range(1, groups):
            out.append(lax.ppermute(pieces[k], "mode", exchange[k]))
        return out

    def hop(value, pairs):
        return lax.ppermute(value, "mesh", pairs)

    *packed, mag = pack(
        stay(velocity.reshape(6 * modes, nodes)), stay(magnetic.reshape(6 * modes, nodes)), groups
    )
    spread_in = swap(packed)
    fwd, bwd = tables(groups, modes)
    square, joint, send, front, sep_source, rows = compose(
        front_rows, leaf_inverse, leaf_coupling, separator_inverse, separator_coupling, separator_source
    )
    azi = swap(transform(fwd, bwd, spread_in, (1,)))
    lift = hop(send, [(0, mid)])
    rest = transform(fwd, bwd, spread_in, (0, 2))
    rest = swap(rest)
    source, update = leaf_up(rows, mag, azi, joint)
    local = leaf_local(source, square)
    nonlinear = spread(azi, rest).reshape(3, 2, modes, nodes)

    of_level = [[q for q in range(partitions) if level_of(q, levels) == h] for h in range(levels + 2)]
    wide = jax.ShapeDtypeStruct(separator_source.shape, F32)
    half = jax.ShapeDtypeStruct(separator_source.shape, BF16)
    reduced = [None] * (levels + 1)
    one, two = update, hop(update, [(q - 1, q) for q in of_level[1]])
    for height in range(1, levels):
        reduced[height], outgoing = small_call(rise_kernel, [wide, wide], [one, two, sep_source, front])
        gap = 2 ** (height - 1)
        one = hop(outgoing, [(q - gap, q) for q in of_level[height + 1]])
        two = hop(outgoing, [(q + gap, q) for q in of_level[height + 1]])
    x, x16, top = small_call(
        functools.partial(crown_kernel, mid), [wide, half, wide], [one, two, sep_source, front, lift]
    )
    far = hop(top, [(mid, 0)])
    answers = [x, far]
    for height in range(levels - 1, 0, -1):
        gap = 2 ** (height - 1)
        one = hop(x16, [(q, q - gap) for q in of_level[height + 1]])
        two = hop(x16, [(q, q + gap) for q in of_level[height + 1]])
        x, x16 = small_call(sink_kernel, [wide, half], [one, two, reduced[height], front])
        answers.insert(0, x)
    beside = hop(x16, [(q, q - 1) for q in of_level[1]])
    azimuthal, solution = leaf_down(rows, x16, beside, local, joint, answers)
    return (nonlinear, azimuthal, solution)


def solution(mesh):
    in_specs = (
        P(None, None, "mode", "mesh"),
        P(None, None, "mode", "mesh"),
        P("mode", "mesh", None, None),
        P("mode", None, "mesh"),
        P("mode", "mesh", None),
        P("mode", "mesh", None),
        P(None, "mode", "mesh"),
        P("mesh", None, None),
    )
    out_specs = (P(None, None, "mode", "mesh"), P(None, "mode", "mesh"), P(None, "mode", "mesh"))


    return jax.shard_map(shards, mesh=mesh, in_specs=in_specs, out_specs=out_specs, check_vma=False)
```
